32 devices in a mesh: gx: 2 (over x), gy: 4 (over y, core), gz: 4 (over z).
Axes of the slice: x: 2, y: 2, z: 4, core: 2. Of those that a mesh axis runs over, the one named last changes fastest.
Arguments:
- atom_feat: bfloat16 [32768, 128], P(('gx', 'gy', 'gz')), may hold values from -6 to 6
- atom_env: bfloat16 [32768, 9, 128], P(('gx', 'gy', 'gz')), may hold values from -6 to 6
- export_index: int32 [8192], P(('gx', 'gy', 'gz')), may hold values from 0 to 1023
- pair_vec: float32 [3, 65536], P(None, ('gx', 'gy', 'gz')), may hold values from -8 to 8
- pair_center: int32 [65536], P(('gx', 'gy', 'gz')), may hold values from 0 to 1023
- pair_owner: int32 [65536, 1], P(('gx', 'gy', 'gz')), may hold values from 0 to 15; in each aligned block of 2048 rows (0 to 2047, 2048 to 4095, ...) at most 192 rows name the same one
- pair_neigh: int32 [65536], P(('gx', 'gy', 'gz')), may hold values from 0 to 7935
- pair_count: int32 [32], P(('gx', 'gy', 'gz')), may hold values from 512 to 2048
- center_proj: bfloat16 [128, 512], replicated, may hold values from -0.375 to 0.375
- neighbour_proj: bfloat16 [128, 512], replicated, may hold values from -0.375 to 0.375
- radial_proj: bfloat16 [8, 512], replicated, may hold values from -4 to 4
- hidden_proj: bfloat16 [512, 512], replicated, may hold values from -0.25 to 0.25
- split_proj: bfloat16 [512, 384], replicated, may hold values from -0.5 to 0.5
- scalar_proj: bfloat16 [384, 512], replicated, may hold values from -0.3125 to 0.3125
- path_gain: float32 [3, 128], replicated, may hold values from 0.1 to 1.9
- energy_proj: float32 [512], replicated, may hold values from -0.5 to 0.5
Outputs:
- pair_latent: bfloat16 [65536, 512], P(('gx', 'gy', 'gz'))
- pair_vector: bfloat16 [3, 65536, 128], P(None, ('gx', 'gy', 'gz'))
- atom_energy: float32 [32768], P(('gx', 'gy', 'gz'))
The draws below stay inside these ranges and needn't reach their ends.
Inputs may be any that keep to these rules, and one draw needn't show every extreme that they name: `pair_owner`: among the pair slots of one device at most 192 name the same owner, a bound that some block reaches of them.
All inputs are finite; a program needn't handle non-finite values.
Results may differ from the reference program's by a relative error of at most 0.0062.
Values may be sent and summed in bfloat16 or wider, within the bound.
No kernel may reach another device: no remote copies, remote signals or barrier semaphores. Data moves between devices by JAX's collectives and lax.ppermute only.
A program may use at most 128 MiB of HBM per device.

```python
import math
import jax
import jax.numpy as jnp
import numpy as np
from jax import lax

CHANNELS = 128
LATENT = 512
BASIS = 8
ATOMS_DEV = 1024
EXPORT = 256
PAIRS_DEV = 2048
CAPACITY = 192
ATOMS = 32768
PAIRS = 65536
TABLE = 7936
N_GX = 2
N_GY = 4
N_GZ = 4
DEVICES = 32


def set_ends(entries, key, smallest, top_value):
    extent = entries.shape
    spot = [jax.random.randint(jax.random.fold_in(key, axis), (), 0, extent[axis]) for axis in range(len(extent))]
    entries = entries.at[tuple(spot)].set(smallest)
    longest = extent.index(max(extent))
    spot[longest] = (spot[longest] + 1) % extent[longest]
    return entries.at[tuple(spot)].set(top_value)


def level_of(key, dims, cuts, smallest, largest):
    loudness = 1.0
    for position, parts in cuts:
        heights = jax.random.uniform(jax.random.fold_in(jax.random.fold_in(key, 6), position), (parts,), jnp.float32, smallest / len(cuts), largest / len(cuts))
        loudness = loudness * jnp.repeat(jnp.exp(heights), dims[position] // parts).reshape((-1,) + (1,) * (len(dims) - 1 - position))
    return loudness


def routed_block(stream_key, own, number, rows, count, top, limit, lean):
    order = jax.random.permutation(stream_key, count)
    crowded, usual = load_shares(count, rows * top, limit, lean, True), load_shares(count, rows * top, limit, lean, False)
    places = jnp.arange(count)

    def named(sizes, turn):
        used = int((sizes > 0).sum())
        fixed = max(1, used // 4)
        moved = fixed + (places - fixed + turn * (used - fixed)) % max(1, count - fixed)
        return jnp.zeros((count,), jnp.int32).at[order[jnp.where(places < fixed, places, moved)]].set(jnp.asarray(sizes, jnp.int32))

    sizes = jnp.where(number % 4 == 0, named(crowded, number // 4), named(usual, number - number // 4 - 1))
    mixed = jax.random.permutation(jax.random.fold_in(own, 3), count)
    donor, taker = mixed[0:count // 2 * 2:2], mixed[1:count // 2 * 2:2]
    margin = jnp.minimum(sizes[donor] - 1, limit - sizes[taker]) // 2
    margin = jnp.where((donor == order[0]) | (taker == order[0]) | (sizes[taker] == 0), 0, jnp.maximum(margin, 0))
    moved = jax.random.randint(jax.random.fold_in(own, 4), (count // 2,), 0, 1 << 20) % (margin + 1)
    sizes = sizes.at[donor].add(-moved).at[taker].add(moved)
    members = jnp.searchsorted(jnp.cumsum(sizes), jnp.arange(rows * top), side="right").astype(jnp.int32)
    table = members.reshape(top, rows).T
    table = table[jax.random.permutation(jax.random.fold_in(own, 1), rows)]
    turn = jax.random.randint(jax.random.fold_in(own, 2), (rows, 1), 0, top)
    return jnp.take_along_axis(table, (jnp.arange(top)[None, :] + turn) % top, axis=1)


def load_shares(number_of, total, most, lean, full):
    loads = [(1 << 20) // math.isqrt(rank ** lean) + 1 for rank in range(1, number_of + 1)]
    largest = most if full else min(most, max(-(-total // number_of), total * loads[0] // sum(loads)))
    least = 1 if total - largest >= number_of - 1 else 0
    given, surplus = [largest] + [least] * (number_of - 1), total - largest - least * (number_of - 1)
    while surplus > 0:
        movable = [i for i in range(1, number_of) if given[i] < largest] or [i for i in range(1, number_of) if given[i] < most]
        mass, budget = sum([loads[i] for i in movable]), surplus
        for i in movable:
            extra = min(most - given[i], max(1, budget * loads[i] // mass), surplus)
            given[i] = given[i] + extra
            surplus = surplus - extra
    return np.array(given)


def normal_values(own_key, shape, spread, reach, pieces=(), held_as=jnp.bfloat16):
    drawn = spread * jax.random.normal(own_key, shape, jnp.float32)
    if pieces:
        drawn = drawn * level_of(own_key, shape, pieces, -0.22, 0.18)
    return jnp.clip(drawn, -reach, reach).astype(held_as)


def setup_inputs(seed: int = 0) -> dict:
    splits = jax.random.split(jax.random.key(seed), 17)
    atom_feat = normal_values(splits[0], (ATOMS, CHANNELS), 1.0, 6.0, ((0, 32),))
    atom_env = normal_values(splits[1], (ATOMS, 9, CHANNELS), 1.0, 6.0, ((0, 32),))
    export_index = set_ends(jax.random.randint(splits[2], (DEVICES * EXPORT,), 0, ATOMS_DEV), jax.random.fold_in(splits[2], 1), 0, ATOMS_DEV - 1).astype(jnp.int32)
    pair_vec = normal_values(splits[3], (3, PAIRS), 2.0, 8.0, ((1, 32),), jnp.float32)
    pair_center = set_ends(jax.random.randint(splits[4], (PAIRS,), 0, ATOMS_DEV), jax.random.fold_in(splits[4], 1), 0, ATOMS_DEV - 1).astype(jnp.int32)
    pair_owner_keys = jax.random.split(jax.random.fold_in(splits[5], 1), PAIRS // PAIRS_DEV)
    pair_owner_turns = jax.random.permutation(jax.random.fold_in(splits[5], 3), PAIRS // PAIRS_DEV)
    pair_owner = jax.vmap(lambda own, number: routed_block(jax.random.fold_in(splits[5], 2), own, number, PAIRS_DEV, N_GY * N_GZ, 1, CAPACITY, 1))(pair_owner_keys, pair_owner_turns).reshape((PAIRS, 1))
    pair_neigh = set_ends(jax.random.randint(splits[6], (PAIRS,), 0, TABLE), jax.random.fold_in(splits[6], 1), 0, TABLE - 1).astype(jnp.int32)
    pair_count = set_ends(jax.random.randint(splits[7], (DEVICES,), PAIRS_DEV // 4, PAIRS_DEV + 1), jax.random.fold_in(splits[7], 1), PAIRS_DEV // 4, PAIRS_DEV).astype(jnp.int32)
    center_proj = normal_values(splits[8], (CHANNELS, LATENT), (2 * CHANNELS) ** -0.5, 0.375)
    neighbour_proj = normal_values(splits[9], (CHANNELS, LATENT), (2 * CHANNELS) ** -0.5, 0.375)
    radial_proj = normal_values(splits[10], (BASIS, LATENT), 2 ** -0.5, 4.0)
    hidden_proj = normal_values(splits[11], (LATENT, LATENT), LATENT ** -0.5, 0.25)
    split_proj = normal_values(splits[12], (LATENT, 3 * CHANNELS), (LATENT // 4) ** -0.5, 0.5)
    scalar_proj = normal_values(splits[13], (3 * CHANNELS, LATENT), (3 * CHANNELS) ** -0.5, 0.3125)
    path_gain = jnp.clip(1.0 + 0.18 * jax.random.normal(splits[14], (3, CHANNELS), jnp.float32), 0.1, 1.9)
    energy_proj = normal_values(splits[15], (LATENT,), (LATENT // 4) ** -0.5, 0.5, (), jnp.float32)
    return dict(atom_feat=atom_feat, atom_env=atom_env, export_index=export_index, pair_vec=pair_vec, pair_center=pair_center, pair_owner=pair_owner, pair_neigh=pair_neigh, pair_count=pair_count, center_proj=center_proj, neighbour_proj=neighbour_proj, radial_proj=radial_proj, hidden_proj=hidden_proj, split_proj=split_proj, scalar_proj=scalar_proj, path_gain=path_gain, energy_proj=energy_proj)


cutoff = 6.0
root_two = 2.0 ** 0.5
root_three = 3.0 ** 0.5
root_five = 5.0 ** 0.5
root_fifteen = 15.0 ** 0.5

def harmonics(unit):
    ux, uy, uz = (unit[0], unit[1], unit[2])
    first = root_three * unit
    second = jnp.stack([root_fifteen * ux * uy, root_fifteen * uy * uz, 0.5 * root_five * (2.0 * uz * uz - ux * ux - uy * uy), root_fifteen * ux * uz, 0.5 * root_fifteen * (ux * ux - uy * uy)])
    return (first, second)

def pair_block(h_center, env_center, h_neighbour, geometry, live, center_proj, neighbour_proj, radial_proj, hidden_proj, split_proj, scalar_proj, path_gain, energy_proj):
    channels = h_center.shape[1]
    basis = radial_proj.shape[0]
    length = jnp.sqrt(lax.optimization_barrier(jnp.sum(geometry * geometry, axis=0)))
    unit = geometry / jnp.maximum(length, 1.0)[None, :]
    spacing = cutoff / (basis - 1)
    centres = jnp.arange(basis).astype(geometry.dtype) * spacing
    radial = jnp.exp(-jnp.square((length[:, None] - centres[None, :]) / spacing))
    before = jnp.dot(h_center, center_proj, preferred_element_type=jnp.float32)
    before = before + jnp.dot(h_neighbour, neighbour_proj, preferred_element_type=jnp.float32)
    before = before + jnp.dot(radial, radial_proj.astype(jnp.float32), precision=lax.Precision.HIGHEST)
    hidden = jax.nn.silu(before).astype(jnp.bfloat16)
    latent = jax.nn.silu(jnp.dot(hidden, hidden_proj, preferred_element_type=jnp.float32)).astype(jnp.bfloat16)
    mixed = jnp.dot(latent, split_proj, preferred_element_type=jnp.float32)
    scalar_part = mixed[:, :channels]
    vector_part = mixed[:, channels:2 * channels]
    tensor_part = mixed[:, 2 * channels:]
    first, second = harmonics(unit)
    envelope = env_center.astype(jnp.float32)
    env_scalar = envelope[:, 0, :]
    env_vector = jnp.moveaxis(envelope[:, 1:4, :], 1, 0)
    env_tensor = jnp.moveaxis(envelope[:, 4:9, :], 1, 0)
    edge_vector = vector_part[None] * first[:, :, None]
    edge_tensor = tensor_part[None] * second[:, :, None]
    invariants = jnp.concatenate([scalar_part * env_scalar, lax.optimization_barrier(jnp.sum(edge_vector * env_vector, axis=0)) / root_three, lax.optimization_barrier(jnp.sum(edge_tensor * env_tensor, axis=0)) / root_five], axis=1).astype(jnp.bfloat16)
    update = jax.nn.silu(jnp.dot(invariants, scalar_proj, preferred_element_type=jnp.float32))
    latent_out = jnp.where(live[:, None], latent.astype(jnp.float32) + update, 0.0).astype(jnp.bfloat16)
    cross = jnp.stack([edge_vector[1] * env_vector[2] - edge_vector[2] * env_vector[1], edge_vector[2] * env_vector[0] - edge_vector[0] * env_vector[2], edge_vector[0] * env_vector[1] - edge_vector[1] * env_vector[0]])
    vector_out = path_gain[0][None, None, :] * scalar_part[None] * env_vector + path_gain[1][None, None, :] * edge_vector * env_scalar[None] + path_gain[2][None, None, :] * cross / root_two
    vector_out = jnp.where(live[None, :, None], vector_out, 0.0).astype(jnp.bfloat16)
    energy = lax.optimization_barrier(jnp.sum(latent_out.astype(jnp.float32) * energy_proj[None, :], axis=1))
    energy = jnp.where(live, energy, 0.0)
    return (latent_out, vector_out, energy)

def reference(atom_feat, atom_env, export_index, pair_vec, pair_center, pair_owner, pair_neigh, pair_count, center_proj, neighbour_proj, radial_proj, hidden_proj, split_proj, scalar_proj, path_gain, energy_proj):
    devices = N_GX * N_GY * N_GZ
    owners = N_GY * N_GZ
    owner_all = pair_owner[:, 0]

    def one_device(index):
        offset = index * PAIRS_DEV
        geometry = lax.dynamic_slice_in_dim(pair_vec, offset, PAIRS_DEV, 1)
        center = lax.dynamic_slice_in_dim(pair_center, offset, PAIRS_DEV, 0)
        owner = lax.dynamic_slice_in_dim(owner_all, offset, PAIRS_DEV, 0)
        neighbour = lax.dynamic_slice_in_dim(pair_neigh, offset, PAIRS_DEV, 0)
        owner_dev = index // owners * owners + owner
        center_row = owner_dev * ATOMS_DEV + center
        halo_slot = jnp.maximum(neighbour - ATOMS_DEV, 0)
        cell = halo_slot // EXPORT
        member = halo_slot % EXPORT
        source_x = (owner_dev // owners + cell // 9 - 1) % N_GX
        source_y = (owner_dev // N_GZ % N_GY + cell // 3 % 3 - 1) % N_GY
        source_z = (owner_dev % N_GZ + cell % 3 - 1) % N_GZ
        source = (source_x * N_GY + source_y) * N_GZ + source_z
        halo_row = source * ATOMS_DEV + export_index[source * EXPORT + member]
        neighbour_row = jnp.where(neighbour < ATOMS_DEV, owner_dev * ATOMS_DEV + neighbour, halo_row)
        live = jnp.arange(PAIRS_DEV, dtype=jnp.int32) < pair_count[index]
        latent_out, vector_out, energy = pair_block(atom_feat[center_row], atom_env[center_row], atom_feat[neighbour_row], geometry, live, center_proj, neighbour_proj, radial_proj, hidden_proj, split_proj, scalar_proj, path_gain, energy_proj)
        return (latent_out, vector_out, energy, center_row)
    latent_all, vector_all, energy_all, rows_all = lax.map(one_device, jnp.arange(devices, dtype=jnp.int32))
    pair_latent = latent_all.reshape(devices * PAIRS_DEV, latent_all.shape[-1])
    pair_vector = jnp.moveaxis(vector_all, 1, 0).reshape(3, devices * PAIRS_DEV, vector_all.shape[-1])
    atom_energy = jax.ops.segment_sum(energy_all.reshape(-1), rows_all.reshape(-1), num_segments=devices * ATOMS_DEV)
    return (pair_latent, pair_vector, atom_energy)
```

```python
import functools

import jax
import jax.numpy as jnp
from jax import lax
from jax.experimental import pallas as pl
from jax.experimental.pallas import tpu as pltpu
from jax.sharding import PartitionSpec as P

cutoff = 6.0
root_two = 2.0**0.5
root_three = 3.0**0.5
root_five = 5.0**0.5
root_fifteen = 15.0**0.5
f32 = jnp.float32
bf16 = jnp.bfloat16
LANES = 128
NT = (((1,), (1,)), ((), ()))


def split3(v):
    high = v.astype(bf16).astype(f32)
    rest = v - high
    middle = rest.astype(bf16).astype(f32)
    return (high, middle, rest - middle)


def route_kernel(owners, cap, count_ref, owner_ref, center_ref, vec_ref, rows_ref, request_ref):
    slots = owner_ref.shape[1]
    padded = request_ref.shape[2]
    owner = owner_ref[...]
    center = center_ref[...]
    member = owner == lax.broadcasted_iota(jnp.int32, (owners, slots), 0)
    member = jnp.where(member, 1.0, 0.0)
    step = 256
    before = lax.broadcasted_iota(jnp.int32, (step, step), 0) < lax.broadcasted_iota(
        jnp.int32, (step, step), 1
    )
    before = jnp.where(before, 1.0, 0.0).astype(bf16)
    seen = jnp.zeros((owners, 1), f32)
    ranks = []
    for start in range(0, slots, step):
        part = member[:, start : start + step]
        earlier = jnp.dot(part.astype(bf16), before, preferred_element_type=f32) + seen
        ranks.append(jnp.sum(part * earlier, axis=0, keepdims=True))
        seen = seen + jnp.sum(part, axis=1, keepdims=True)
    rank = jnp.concatenate(ranks, axis=1)
    position = lax.broadcasted_iota(jnp.int32, (1, slots), 1)
    live = jnp.where(position < count_ref[0], 1.0, 0.0)
    vec = vec_ref[...]
    length = jnp.sqrt(jnp.sum(vec * vec, axis=0, keepdims=True))
    unit = vec / jnp.maximum(length, 1.0)
    rows_ref[0:3, :] = root_three * unit
    rows_ref[3:4, :] = live
    rows_ref[4:5, :] = owner.astype(f32) * cap + rank
    rows_ref[5:6, :] = owner.astype(f32)
    rows_ref[6:7, :] = center.astype(f32)
    rows_ref[7:8, :] = length
    code = center + 1
    values = [(code // 256).astype(f32), (code % 256).astype(f32)]
    for m in range(3):
        values.extend(split3(vec[m : m + 1, :]))
    listed = member * live
    left = jnp.concatenate([(listed * v).astype(bf16) for v in values], axis=0)
    place = rank.astype(jnp.int32) == lax.broadcasted_iota(jnp.int32, (padded, slots), 0)
    place = jnp.where(place, 1.0, 0.0).astype(bf16)
    sent = lax.dot_general(left, place, NT, preferred_element_type=f32)
    at = lambda i: sent[i * owners : (i + 1) * owners, :]
    request_ref[:, 0, :] = 256.0 * at(0) + at(1)
    for m in range(3):
        request_ref[:, 1 + m, :] = at(2 + 3 * m) + at(3 + 3 * m) + at(4 + 3 * m)


def owner_kernel(cap, request_ref, env_ref, out_ref, table_ref):
    group = request_ref.shape[0]
    components, atoms, channels = env_ref.shape

    @pl.when(pl.program_id(0) == 0)
    def _():
        for m in range(components):
            table_ref[:, m * channels : (m + 1) * channels] = env_ref[m]

    masks = []
    weights = []
    for g in range(group):
        block = request_ref[g]
        code, vec = (block[0:1, :], block[1:4, :])
        length = jnp.sqrt(jnp.sum(vec * vec, axis=0, keepdims=True))
        unit = vec / jnp.maximum(length, 1.0)
        ux, uy, uz = (unit[0:1], unit[1:2], unit[2:3])
        rows = jnp.concatenate(
            [
                code,
                root_fifteen * ux * uy,
                root_fifteen * uy * uz,
                0.5 * root_five * (2.0 * uz * uz - ux * ux - uy * uy),
                root_fifteen * ux * uz,
                0.5 * root_fifteen * (ux * ux - uy * uy),
                jnp.zeros_like(code),
                jnp.zeros_like(code),
            ],
            axis=0,
        )
        columns = jnp.transpose(rows)[:cap]
        atom = lax.broadcasted_iota(jnp.int32, (cap, atoms), 1) + 1
        hit = columns[:, 0:1].astype(jnp.int32) == atom
        masks.append(jnp.where(hit, 1.0, 0.0).astype(bf16))
        weights.append(columns)
    pick = jnp.concatenate(masks, axis=0)
    weight = jnp.concatenate(weights, axis=0)
    found = jnp.dot(pick, table_ref[...], preferred_element_type=f32)
    keep = 4 * channels
    out_ref[:, :keep] = found[:, :keep].astype(bf16)
    total = weight[:, 1:2] * found[:, keep : keep + channels]
    for m in range(1, 5):
        start = keep + m * channels
        total = total + weight[:, 1 + m : 2 + m] * found[:, start : start + channels]
    out_ref[:, keep:] = total.astype(bf16)


def final_kernel(
    owners,
    rows_ref,
    env_ref,
    mixed_ref,
    latent_ref,
    scalar_ref,
    gain_ref,
    energy_ref,
    latent_out_ref,
    vector_out_ref,
    sums_ref,
):
    many = rows_ref.shape[1]
    places = env_ref.shape[0]
    channels = gain_ref.shape[1]
    atoms = sums_ref.shape[1]
    columns = jnp.transpose(rows_ref[...])
    slot = columns[:, 4:5].astype(jnp.int32)
    hit = slot == lax.broadcasted_iota(jnp.int32, (many, places), 1)
    pick = jnp.where(hit, 1.0, 0.0).astype(bf16)
    env = jnp.dot(pick, env_ref[...], preferred_element_type=f32)
    part = lambda i: env[:, i * channels : (i + 1) * channels]
    env_scalar, env_vector, tensor = (part(0), [part(1), part(2), part(3)], part(4))
    mixed = mixed_ref[...]
    scalar_part = mixed[:, :channels]
    vector_part = mixed[:, channels : 2 * channels]
    tensor_part = mixed[:, 2 * channels :]
    edge = [vector_part * columns[:, m : m + 1] for m in range(3)]
    vector_dot = edge[0] * env_vector[0] + edge[1] * env_vector[1] + edge[2] * env_vector[2]
    invariants = jnp.concatenate(
        [
            (scalar_part * env_scalar).astype(bf16),
            (vector_dot * (1.0 / root_three)).astype(bf16),
            (tensor_part * tensor * (1.0 / root_five)).astype(bf16),
        ],
        axis=1,
    )
    live = columns[:, 3:4] > 0.5
    cross = [
        edge[1] * env_vector[2] - edge[2] * env_vector[1],
        edge[2] * env_vector[0] - edge[0] * env_vector[2],
        edge[0] * env_vector[1] - edge[1] * env_vector[0],
    ]
    gain = gain_ref[...]
    for m in range(3):
        value = (
            gain[0:1] * scalar_part * env_vector[m]
            + gain[1:2] * edge[m] * env_scalar
            + (gain[2:3] * (1.0 / root_two)) * cross[m]
        )
        vector_out_ref[m] = jnp.where(live, value, 0.0).astype(bf16)
    update = jnp.dot(invariants, scalar_ref[...], preferred_element_type=f32)
    update = update * jax.nn.sigmoid(update)
    latent = jnp.where(live, latent_ref[...].astype(f32) + update, 0.0).astype(bf16)
    latent_out_ref[...] = latent
    energy = jnp.sum(latent.astype(f32) * energy_ref[...], axis=1, keepdims=True)
    lane = lax.broadcasted_iota(jnp.int32, (many, LANES), 1)
    owner = columns[:, 5:6].astype(jnp.int32)
    spread = jnp.zeros((many, LANES), f32)
    for i, piece in enumerate(split3(energy)):
        spread = spread + jnp.where(lane == owner + i * owners, piece, 0.0)
    spread = jnp.transpose(spread).astype(bf16)
    center = columns[:, 6:7].astype(jnp.int32)
    of_atom = center == lax.broadcasted_iota(jnp.int32, (many, atoms), 1)
    of_atom = jnp.where(of_atom, 1.0, 0.0).astype(bf16)
    sums = jnp.dot(spread, of_atom, preferred_element_type=f32)
    sums = sums[:owners] + sums[owners : 2 * owners] + sums[2 * owners : 3 * owners]

    @pl.when(pl.program_id(0) == 0)
    def _():
        sums_ref[...] = sums

    @pl.when(pl.program_id(0) > 0)
    def _():
        sums_ref[...] = sums_ref[...] + sums


def whole(shape):
    return pl.BlockSpec(shape, lambda *_: (0,) * len(shape))


def swap(x, axis, bit):
    return lax.ppermute(x, axis, [(i, i ^ bit) for i in range(lax.axis_size(axis))])


def local(
    atom_feat,
    atom_env,
    export_index,
    pair_vec,
    pair_center,
    pair_owner,
    pair_neigh,
    pair_count,
    center_proj,
    neighbour_proj,
    radial_proj,
    hidden_proj,
    split_proj,
    scalar_proj,
    path_gain,
    energy_proj,
):
    atoms, channels = atom_feat.shape
    slots = pair_center.shape[0]
    exports = export_index.shape[0]
    latent_width = hidden_proj.shape[1]
    nx, ny, nz = (lax.axis_size("gx"), lax.axis_size("gy"), lax.axis_size("gz"))
    owners = ny * nz
    cap = 3 * slots // (2 * owners)
    padded = -(-cap // LANES) * LANES
    components = atom_env.shape[1]

    exported = atom_feat[export_index]
    up = [(i, (i + 1) % nx) for i in range(nx)]
    down = [(j, i) for i, j in up]
    parts = [atom_feat, exported, lax.ppermute(exported, "gx", up)]
    if nx > 2:
        parts.append(lax.ppermute(exported, "gx", down))
    block = jnp.concatenate(parts, axis=0)
    block_rows = block.shape[0]
    table = jnp.stack([block] + [swap(block, "gz", k) for k in range(1, nz)])
    bit = ny // 2
    while bit:
        table = jnp.stack([table, swap(table, "gy", bit)])
        bit //= 2
    bits = ny.bit_length() - 1
    table = table.reshape(-1, channels)

    rows, request = pl.pallas_call(
        functools.partial(route_kernel, owners, cap),
        out_shape=(
            jax.ShapeDtypeStruct((8, slots), f32),
            jax.ShapeDtypeStruct((owners, 4, padded), f32),
        ),
        in_specs=[pl.BlockSpec(memory_space=pltpu.SMEM)]
        + [pl.BlockSpec(memory_space=pltpu.VMEM)] * 3,
        out_specs=[pl.BlockSpec(memory_space=pltpu.VMEM)] * 2,
        name="route",
    )(pair_count, pair_owner.reshape(1, slots), pair_center.reshape(1, slots), pair_vec)
    request = lax.all_to_all(request, ("gy", "gz"), split_axis=0, concat_axis=0, tiled=True)

    group = min(4, owners)
    env = jnp.transpose(atom_env, (1, 0, 2))
    sent = pl.pallas_call(
        functools.partial(owner_kernel, cap),
        grid=(owners // group,),
        out_shape=jax.ShapeDtypeStruct((owners * cap, 5 * channels), bf16),
        in_specs=[
            pl.BlockSpec((group, 4, padded), lambda i: (i, 0, 0)),
            whole((components, atoms, channels)),
        ],
        out_specs=pl.BlockSpec((group * cap, 5 * channels), lambda i: (i, 0)),
        scratch_shapes=[pltpu.VMEM((atoms, components * channels), bf16)],
        compiler_params=pltpu.CompilerParams(dimension_semantics=("arbitrary",)),
        name="owner",
    )(request, env)
    received = lax.all_to_all(
        sent.reshape(owners, cap, 5 * channels),
        ("gy", "gz"),
        split_axis=0,
        concat_axis=0,
        tiled=True,
    ).reshape(owners * cap, 5 * channels)

    owner = pair_owner[:, 0]
    oy, oz = (owner // nz, owner % nz)
    my_y, my_z = (lax.axis_index("gy"), lax.axis_index("gz"))

    def place(y, z):
        dy, dz = (y ^ my_y, z ^ my_z)
        flipped = jnp.zeros_like(dy)
        for b in range(bits):
            flipped = flipped | (((dy >> b) & 1) << (bits - 1 - b))
        return (flipped * nz + dz) * block_rows

    center_at = place(oy, oz) + pair_center
    k = jnp.maximum(pair_neigh - atoms, 0)
    cell, member = (k // exports, k % exports)
    dx, dy, dz = (cell // 9 - 1, cell // 3 % 3 - 1, cell % 3 - 1)
    sy, sz = ((oy + dy) % ny, (oz + dz) % nz)
    if nx > 2:
        which = jnp.where(dx == 0, 0, jnp.where(dx < 0, 1, 2))
    else:
        which = jnp.where(dx == 0, 0, 1)
    halo_at = place(sy, sz) + atoms + which * exports + member
    neighbour_at = jnp.where(pair_neigh < atoms, place(oy, oz) + pair_neigh, halo_at)
    pair_feat = jnp.concatenate([table[center_at], table[neighbour_at]], axis=1)
    length = rows[7]
    basis = radial_proj.shape[0]
    spacing = cutoff / (basis - 1)
    centres = jnp.arange(basis).astype(f32) * spacing
    radial = jnp.exp(-jnp.square((length[:, None] - centres[None, :]) / spacing))
    both = jnp.concatenate([center_proj, neighbour_proj], axis=0)
    before = jnp.dot(pair_feat, both, preferred_element_type=f32)
    before = before + jnp.dot(radial, radial_proj.astype(f32), precision=lax.Precision.HIGHEST)
    hidden = jax.nn.silu(before).astype(bf16)
    latent = jax.nn.silu(jnp.dot(hidden, hidden_proj, preferred_element_type=f32)).astype(bf16)
    mixed = jnp.dot(latent, split_proj, preferred_element_type=f32)

    many = min(512, slots)
    latent_out, vector_out, sums = pl.pallas_call(
        functools.partial(final_kernel, owners),
        grid=(slots // many,),
        out_shape=(
            jax.ShapeDtypeStruct((slots, latent_width), bf16),
            jax.ShapeDtypeStruct((3, slots, channels), bf16),
            jax.ShapeDtypeStruct((owners, atoms), f32),
        ),
        in_specs=[
            pl.BlockSpec((8, many), lambda i: (0, i)),
            whole((owners * cap, 5 * channels)),
            pl.BlockSpec((many, 3 * channels), lambda i: (i, 0)),
            pl.BlockSpec((many, latent_width), lambda i: (i, 0)),
            whole(scalar_proj.shape),
            whole(path_gain.shape),
            whole((1, latent_width)),
        ],
        out_specs=(
            pl.BlockSpec((many, latent_width), lambda i: (i, 0)),
            pl.BlockSpec((3, many, channels), lambda i: (0, i, 0)),
            whole((owners, atoms)),
        ),
        compiler_params=pltpu.CompilerParams(dimension_semantics=("arbitrary",)),
        name="final",
    )(rows, received, mixed, latent, scalar_proj, path_gain, energy_proj.reshape(1, latent_width))
    sums = lax.all_to_all(sums, ("gy", "gz"), split_axis=0, concat_axis=0, tiled=True)
    return (latent_out, vector_out, jnp.sum(sums, axis=0))


def solution(mesh):
    placed = (
        P(("gx", "gy", "gz"), None),
        P(("gx", "gy", "gz"), None, None),
        P(("gx", "gy", "gz")),
        P(None, ("gx", "gy", "gz")),
        P(("gx", "gy", "gz")),
        P(("gx", "gy", "gz"), None),
        P(("gx", "gy", "gz")),
        P(("gx", "gy", "gz")),
        P(),
        P(),
        P(),
        P(),
        P(),
        P(),
        P(),
        P(),
    )
    return jax.shard_map(
        local,
        mesh=mesh,
        in_specs=placed,
        out_specs=(
            P(("gx", "gy", "gz"), None),
            P(None, ("gx", "gy", "gz"), None),
            P(("gx", "gy", "gz")),
        ),
        check_vma=False,
    )
```

```python
import functools

import jax
import jax.numpy as jnp
from jax import lax
from jax.experimental import pallas as pl
from jax.experimental.pallas import tpu as pltpu
from jax.sharding import PartitionSpec as P


cutoff = 6.0
root_two = 2.0**0.5
root_three = 3.0**0.5
root_five = 5.0**0.5
root_fifteen = 15.0**0.5
f32 = jnp.float32
bf16 = jnp.bfloat16
LANES = 128
STEP = 256
NT = (((1,), (1,)), ((), ()))


def split3(v):
    high = v.astype(bf16).astype(f32)
    rest = v - high
    middle = rest.astype(bf16).astype(f32)
    return (high, middle, rest - middle)


def route_kernel(
    owners,
    cap,
    window,
    count_ref,
    owner_ref,
    center_ref,
    vec_ref,
    export_ref,
    rows_ref,
    starts_ref,
    request_ref,
):
    slots = owner_ref.shape[1]
    padded = request_ref.shape[2]
    owner = owner_ref[...]
    center = center_ref[...]
    member = owner == lax.broadcasted_iota(jnp.int32, (owners, slots), 0)
    member = jnp.where(member, 1.0, 0.0)
    step = STEP
    before = lax.broadcasted_iota(jnp.int32, (step, step), 0) < lax.broadcasted_iota(
        jnp.int32, (step, step), 1
    )
    before = jnp.where(before, 1.0, 0.0).astype(bf16)
    seen = jnp.zeros((owners, 1), f32)
    lane = lax.broadcasted_iota(jnp.int32, starts_ref.shape, 1)
    starts = jnp.zeros(starts_ref.shape, f32)
    ranks = []
    bases = []
    for start in range(0, slots, step):
        part = member[:, start : start + step]
        earlier = jnp.dot(part.astype(bf16), before, preferred_element_type=f32) + seen
        ranks.append(jnp.sum(part * earlier, axis=0, keepdims=True))
        base = jnp.minimum(jnp.floor(seen * (1.0 / 16.0)) * 16.0, cap - window)
        bases.append(jnp.sum(part * base, axis=0, keepdims=True))
        seen = seen + jnp.sum(part, axis=1, keepdims=True)
        starts = jnp.where(lane == start // step + 1, seen, starts)
    starts_ref[...] = starts.astype(jnp.int32)
    rank = jnp.concatenate(ranks, axis=1)
    place_in = owner.astype(f32) * window + rank - jnp.concatenate(bases, axis=1)
    position = lax.broadcasted_iota(jnp.int32, (1, slots), 1)
    live = jnp.where(position < count_ref[0], 1.0, 0.0)
    vec = vec_ref[...]
    length = jnp.sqrt(jnp.sum(vec * vec, axis=0, keepdims=True))
    unit = vec / jnp.maximum(length, 1.0)
    rows_ref[0:3, :] = root_three * unit
    rows_ref[3:4, :] = place_in
    rows_ref[4:5, :] = owner.astype(f32) * cap + rank
    rows_ref[5:6, :] = jnp.where(live > 0.5, owner.astype(f32), -1.0)
    rows_ref[6:7, :] = center.astype(f32)
    rows_ref[7:8, :] = length
    code = center + 1
    values = [(code // 256).astype(f32), (code % 256).astype(f32)]
    for m in range(3):
        values.extend(split3(vec[m : m + 1, :]))
    listed = member * live
    left = jnp.concatenate([(listed * v).astype(bf16) for v in values], axis=0)
    place = rank.astype(jnp.int32) == lax.broadcasted_iota(jnp.int32, (padded, slots), 0)
    place = jnp.where(place, 1.0, 0.0).astype(bf16)
    sent = lax.dot_general(left, place, NT, preferred_element_type=f32)
    at = lambda i: sent[i * owners : (i + 1) * owners, :]
    fields = [256.0 * at(0) + at(1)]
    fields += [at(2 + 3 * m) + at(3 + 3 * m) + at(4 + 3 * m) for m in range(3)]
    exports = export_ref.shape[1]
    exported = export_ref[...].astype(f32)
    free = padded - cap
    if request_ref.shape[1] == 4:
        lane = lax.broadcasted_iota(jnp.int32, (1, padded), 1)
        rest = jnp.concatenate([exported] * (-(-padded // exports)), axis=1)[:, :padded]
        for m in range(4):
            shift = (cap - m * free) % exports
            turned = pltpu.roll(jnp.broadcast_to(rest, (8, padded)), shift, 1)[:1]
            fields[m] = jnp.where(lane >= cap, turned, fields[m])
    for m in range(4):
        request_ref[:, m, :] = fields[m]
    for m in range(4, request_ref.shape[1]):
        piece = exported[:, (m - 4) * padded : (m - 3) * padded]
        request_ref[:, m, :] = jnp.broadcast_to(piece, (owners, padded))


def owner_kernel(cap, request_ref, env_ref, out_ref, table_ref):
    group = request_ref.shape[0]
    components, atoms, channels = env_ref.shape

    @pl.when(pl.program_id(0) == 0)
    def _():
        for m in range(components):
            table_ref[:, m * channels : (m + 1) * channels] = env_ref[m]

    masks = []
    weights = []
    for g in range(group):
        block = request_ref[g]
        code, vec = (block[0:1, :], block[1:4, :])
        length = jnp.sqrt(jnp.sum(vec * vec, axis=0, keepdims=True))
        unit = vec / jnp.maximum(length, 1.0)
        ux, uy, uz = (unit[0:1], unit[1:2], unit[2:3])
        rows = jnp.concatenate(
            [
                code,
                root_fifteen * ux * uy,
                root_fifteen * uy * uz,
                0.5 * root_five * (2.0 * uz * uz - ux * ux - uy * uy),
                root_fifteen * ux * uz,
                0.5 * root_fifteen * (ux * ux - uy * uy),
                jnp.zeros_like(code),
                jnp.zeros_like(code),
            ],
            axis=0,
        )
        columns = jnp.transpose(rows)[:cap]
        atom = lax.broadcasted_iota(jnp.int32, (cap, atoms), 1) + 1
        hit = columns[:, 0:1].astype(jnp.int32) == atom
        masks.append(jnp.where(hit, 1.0, 0.0).astype(bf16))
        weights.append(columns)
    pick = jnp.concatenate(masks, axis=0)
    weight = jnp.concatenate(weights, axis=0)
    found = jnp.dot(pick, table_ref[...], preferred_element_type=f32)
    keep = 4 * channels
    out_ref[:, :keep] = found[:, :keep].astype(bf16)
    total = weight[:, 1:2] * found[:, keep : keep + channels]
    for m in range(1, 5):
        start = keep + m * channels
        total = total + weight[:, 1 + m : 2 + m] * found[:, start : start + channels]
    out_ref[:, keep:] = total.astype(bf16)


def latent_kernel(basis, block_rows, index_ref, lists_ref, rows_ref, *refs):
    pieces = refs[:-8]
    both_ref, radial_ref, hidden_ref, split_ref, latent_ref, mixed_ref = refs[-8:-2]
    table_ref, feat_ref = refs[-2:]
    many, _ = feat_ref.shape[1:]

    @pl.when(pl.program_id(0) == 0)
    def _():
        for i, piece in enumerate(pieces):
            table_ref[i * block_rows : (i + 1) * block_rows, :] = piece[...].astype(f32)

    start = pl.program_id(0) * many
    unroll = 16

    def gather(i, carry):
        at = pl.multiple_of(i * unroll, unroll)
        read = (start + at) * 3
        centers = [index_ref[read + 3 * j] for j in range(unroll)]
        entries = [index_ref[read + 3 * j + 2] for j in range(unroll)]
        neighbours = [index_ref[read + 3 * j + 1] + lists_ref[entries[j]] for j in range(unroll)]
        for j in range(unroll):
            feat_ref[0, pl.ds(at + j, 1), :] = table_ref[pl.ds(centers[j], 1), :]
            feat_ref[1, pl.ds(at + j, 1), :] = table_ref[pl.ds(neighbours[j], 1), :]
        return carry

    lax.fori_loop(0, many // unroll, gather, 0)
    spacing = cutoff / (basis - 1)
    length = rows_ref[7:8, :]
    centres = lax.broadcasted_iota(jnp.int32, (basis, many), 0).astype(f32) * spacing
    scaled = (length - centres) / spacing
    radial = jnp.concatenate(split3(jnp.exp(-(scaled * scaled))), axis=0)
    radial = jnp.transpose(radial).astype(bf16)
    feat = jnp.concatenate([feat_ref[0], feat_ref[1]], axis=1).astype(bf16)
    before = jnp.dot(feat, both_ref[...], preferred_element_type=f32)
    before = before + jnp.dot(radial, radial_ref[...], preferred_element_type=f32)
    hidden = (before * jax.nn.sigmoid(before)).astype(bf16)
    after = jnp.dot(hidden, hidden_ref[...], preferred_element_type=f32)
    latent = (after * jax.nn.sigmoid(after)).astype(bf16)
    latent_ref[...] = latent
    mixed_ref[...] = jnp.dot(latent, split_ref[...], preferred_element_type=f32)


def final_kernel(
    owners,
    cap,
    window,
    starts_ref,
    rows_ref,
    env_ref,
    mixed_ref,
    latent_ref,
    scalar_ref,
    gain_ref,
    energy_ref,
    latent_out_ref,
    vector_out_ref,
    sums_ref,
    near_ref,
    found_ref,
):
    many = rows_ref.shape[1]
    places = env_ref.shape[0]
    channels = gain_ref.shape[1]
    atoms = sums_ref.shape[1]
    columns = jnp.transpose(rows_ref[...])
    step = pl.program_id(0)

    def pick(column, size):
        hit = columns[:, column : column + 1].astype(jnp.int32) == lax.broadcasted_iota(
            jnp.int32, (many, size), 1
        )
        return jnp.where(hit, 1.0, 0.0).astype(bf16)

    fits = True
    bases = []
    for o in range(owners):
        base = jnp.minimum(starts_ref[o, step] // 16 * 16, cap - window)
        bases.append(base)
        fits = fits & (starts_ref[o, step + 1] <= base + window)

    @pl.when(fits)
    def _():
        for o in range(owners):
            at = pl.multiple_of(o * cap + bases[o], 16)
            near_ref[o * window : (o + 1) * window, :] = env_ref[pl.ds(at, window), :]
        found_ref[...] = jnp.dot(
            pick(3, owners * window), near_ref[...], preferred_element_type=f32
        )

    @pl.when(jnp.logical_not(fits))
    def _():
        found_ref[...] = jnp.dot(pick(4, places), env_ref[...], preferred_element_type=f32)

    env = found_ref[...]
    part = lambda i: env[:, i * channels : (i + 1) * channels]
    env_scalar, env_vector, tensor = (part(0), [part(1), part(2), part(3)], part(4))
    mixed = mixed_ref[...]
    scalar_part = mixed[:, :channels]
    vector_part = mixed[:, channels : 2 * channels]
    tensor_part = mixed[:, 2 * channels :]
    edge = [vector_part * columns[:, m : m + 1] for m in range(3)]
    vector_dot = edge[0] * env_vector[0] + edge[1] * env_vector[1] + edge[2] * env_vector[2]
    invariants = jnp.concatenate(
        [
            (scalar_part * env_scalar).astype(bf16),
            (vector_dot * (1.0 / root_three)).astype(bf16),
            (tensor_part * tensor * (1.0 / root_five)).astype(bf16),
        ],
        axis=1,
    )
    live = columns[:, 5:6] >= 0.0
    cross = [
        edge[1] * env_vector[2] - edge[2] * env_vector[1],
        edge[2] * env_vector[0] - edge[0] * env_vector[2],
        edge[0] * env_vector[1] - edge[1] * env_vector[0],
    ]
    gain = gain_ref[...]
    for m in range(3):
        value = (
            gain[0:1] * scalar_part * env_vector[m]
            + gain[1:2] * edge[m] * env_scalar
            + (gain[2:3] * (1.0 / root_two)) * cross[m]
        )
        vector_out_ref[m] = jnp.where(live, value, 0.0).astype(bf16)
    update = jnp.dot(invariants, scalar_ref[...], preferred_element_type=f32)
    update = update * jax.nn.sigmoid(update)
    latent = jnp.where(live, latent_ref[...].astype(f32) + update, 0.0).astype(bf16)
    latent_out_ref[...] = latent
    energy = jnp.sum(latent.astype(f32) * energy_ref[...], axis=1, keepdims=True)
    lane = lax.broadcasted_iota(jnp.int32, (many, LANES), 1)
    owner = columns[:, 5:6].astype(jnp.int32)
    spread = jnp.zeros((many, LANES), f32)
    for i, piece in enumerate(split3(energy)):
        spread = spread + jnp.where(lane == owner + i * owners, piece, 0.0)
    spread = jnp.transpose(spread).astype(bf16)
    center = columns[:, 6:7].astype(jnp.int32)
    of_atom = center == lax.broadcasted_iota(jnp.int32, (many, atoms), 1)
    of_atom = jnp.where(of_atom, 1.0, 0.0).astype(bf16)
    sums = jnp.dot(spread, of_atom, preferred_element_type=f32)
    sums = sums[:owners] + sums[owners : 2 * owners] + sums[2 * owners : 3 * owners]

    @pl.when(pl.program_id(0) == 0)
    def _():
        sums_ref[...] = sums

    @pl.when(pl.program_id(0) > 0)
    def _():
        sums_ref[...] = sums_ref[...] + sums


def whole(shape):
    return pl.BlockSpec(shape, lambda *_: (0,) * len(shape))


def swap(x, axis, bit):
    return lax.ppermute(x, axis, [(i, i ^ bit) for i in range(lax.axis_size(axis))])


def local(
    atom_feat,
    atom_env,
    export_index,
    pair_vec,
    pair_center,
    pair_owner,
    pair_neigh,
    pair_count,
    center_proj,
    neighbour_proj,
    radial_proj,
    hidden_proj,
    split_proj,
    scalar_proj,
    path_gain,
    energy_proj,
):
    atoms, channels = atom_feat.shape
    slots = pair_center.shape[0]
    exports = export_index.shape[0]
    latent_width = hidden_proj.shape[1]
    nx, ny, nz = (lax.axis_size("gx"), lax.axis_size("gy"), lax.axis_size("gz"))
    owners = ny * nz
    cap = 3 * slots // (2 * owners)
    padded = -(-cap // LANES) * LANES
    components = atom_env.shape[1]

    fields = 4 if 4 * (padded - cap) >= exports else 4 + -(-exports // padded)
    window = min(64, cap)
    rows, starts, request = pl.pallas_call(
        functools.partial(route_kernel, owners, cap, window),
        out_shape=(
            jax.ShapeDtypeStruct((8, slots), f32),
            jax.ShapeDtypeStruct((owners, LANES), jnp.int32),
            jax.ShapeDtypeStruct((owners, fields, padded), f32),
        ),
        in_specs=[pl.BlockSpec(memory_space=pltpu.SMEM)]
        + [pl.BlockSpec(memory_space=pltpu.VMEM)] * 4,
        out_specs=[pl.BlockSpec(memory_space=pltpu.VMEM)] * 3,
        name="route",
    )(
        pair_count,
        pair_owner.reshape(1, slots),
        pair_center.reshape(1, slots),
        pair_vec,
        export_index.reshape(1, exports),
    )
    export_index, rows = lax.optimization_barrier((export_index, rows))
    request = lax.all_to_all(request, ("gy", "gz"), split_axis=0, concat_axis=0, tiled=True)

    exported = atom_feat[export_index]
    up = [(i, (i + 1) % nx) for i in range(nx)]
    down = [(j, i) for i, j in up]
    parts = [atom_feat, lax.ppermute(exported, "gx", up)]
    if nx > 2:
        parts.append(lax.ppermute(exported, "gx", down))
    block = jnp.concatenate(parts, axis=0)
    block_rows = block.shape[0]
    block, request = lax.optimization_barrier((block, request))
    pieces = {(0, 0): block}
    for k in range(1, nz):
        pieces[0, k] = swap(block, "gz", k)

    group = min(4, owners)
    env = jnp.transpose(atom_env, (1, 0, 2))
    sent = pl.pallas_call(
        functools.partial(owner_kernel, cap),
        grid=(owners // group,),
        out_shape=jax.ShapeDtypeStruct((owners * cap, 5 * channels), bf16),
        in_specs=[
            pl.BlockSpec((group, fields, padded), lambda i: (i, 0, 0)),
            whole((components, atoms, channels)),
        ],
        out_specs=pl.BlockSpec((group * cap, 5 * channels), lambda i: (i, 0)),
        scratch_shapes=[pltpu.VMEM((atoms, components * channels), bf16)],
        compiler_params=pltpu.CompilerParams(dimension_semantics=("arbitrary",)),
        cost_estimate=pl.CostEstimate(
            flops=2 * owners * cap * atoms * components * channels,
            bytes_accessed=8 * atoms * components * channels,
            transcendentals=0,
        ),
        name="owner",
    )(request, env)
    if fields == 4:
        lists = request[:, :, cap:].reshape(owners, -1)[:, :exports]
    else:
        lists = request[:, 4:, :].reshape(owners, -1)[:, :exports]
    lists, sent = lax.optimization_barrier((lists, sent))
    received = lax.all_to_all(
        sent.reshape(owners, cap, 5 * channels),
        ("gy", "gz"),
        split_axis=0,
        concat_axis=0,
        tiled=True,
    ).reshape(owners * cap, 5 * channels)

    owner = pair_owner[:, 0]
    oy, oz = (owner // nz, owner % nz)
    my_y, my_z = (lax.axis_index("gy"), lax.axis_index("gz"))

    def place(y, z):
        return ((y ^ my_y) * nz + (z ^ my_z)) * block_rows

    k = jnp.maximum(pair_neigh - atoms, 0)
    cell, member = (k // exports, k % exports)
    dx, dy, dz = (cell // 9 - 1, cell // 3 % 3 - 1, cell % 3 - 1)
    sy, sz = ((oy + dy) % ny, (oz + dz) % nz)
    outside = atoms + member
    if nx > 2:
        outside = outside + jnp.where(dx < 0, 0, exports)
    home = place(oy, oz)
    own = pair_neigh < atoms
    listed = (pair_neigh >= atoms) & (dx == 0)
    halo_at = place(sy, sz) + jnp.where(dx == 0, 0, outside)
    entry = jnp.where(listed, (sy * nz + sz) * exports + member + 1, 0)
    lists = jnp.concatenate([jnp.zeros((1,), f32), lists.reshape(-1)]).astype(jnp.int32)
    neighbour_at = jnp.where(own, home + pair_neigh, halo_at)
    index = jnp.stack([home + pair_center, neighbour_at, entry], axis=1).reshape(-1)
    pieces[0, nz - 1], index, lists = lax.optimization_barrier((pieces[0, nz - 1], index, lists))
    bit = ny // 2
    while bit:
        for (y, z), piece in list(pieces.items()):
            pieces[y ^ bit, z] = swap(piece, "gy", bit)
        bit //= 2
    many = min(512, slots)
    basis = radial_proj.shape[0]
    latent, mixed = pl.pallas_call(
        functools.partial(latent_kernel, basis, block_rows),
        grid=(slots // many,),
        out_shape=(
            jax.ShapeDtypeStruct((slots, latent_width), bf16),
            jax.ShapeDtypeStruct((slots, 3 * channels), f32),
        ),
        in_specs=[
            pl.BlockSpec(memory_space=pltpu.SMEM),
            pl.BlockSpec(memory_space=pltpu.SMEM),
            pl.BlockSpec((8, many), lambda i: (0, i)),
        ]
        + [pl.BlockSpec(memory_space=pltpu.VMEM)] * (owners + 4),
        out_specs=(
            pl.BlockSpec((many, latent_width), lambda i: (i, 0)),
            pl.BlockSpec((many, 3 * channels), lambda i: (i, 0)),
        ),
        scratch_shapes=[
            pltpu.VMEM((owners * block_rows, channels), f32),
            pltpu.VMEM((2, many, channels), f32),
        ],
        compiler_params=pltpu.CompilerParams(dimension_semantics=("arbitrary",)),
        cost_estimate=pl.CostEstimate(
            flops=2 * slots * latent_width * (2 * latent_width + 3 * channels),
            bytes_accessed=2 * owners * block_rows * channels,
            transcendentals=4 * slots * latent_width,
        ),
        name="latent",
    )(
        index,
        lists,
        rows,
        *[pieces[i // nz, i % nz] for i in range(owners)],
        jnp.concatenate([center_proj, neighbour_proj], axis=0),
        jnp.concatenate([radial_proj] * 3, axis=0),
        hidden_proj,
        split_proj,
    )

    latent_out, vector_out, sums = pl.pallas_call(
        functools.partial(final_kernel, owners, cap, window),
        grid=(slots // STEP,),
        out_shape=(
            jax.ShapeDtypeStruct((slots, latent_width), bf16),
            jax.ShapeDtypeStruct((3, slots, channels), bf16),
            jax.ShapeDtypeStruct((owners, atoms), f32),
        ),
        in_specs=[
            pl.BlockSpec(memory_space=pltpu.SMEM),
            pl.BlockSpec((8, STEP), lambda i: (0, i)),
            whole((owners * cap, 5 * channels)),
            pl.BlockSpec((STEP, 3 * channels), lambda i: (i, 0)),
            pl.BlockSpec((STEP, latent_width), lambda i: (i, 0)),
            whole(scalar_proj.shape),
            whole(path_gain.shape),
            whole((1, latent_width)),
        ],
        out_specs=(
            pl.BlockSpec((STEP, latent_width), lambda i: (i, 0)),
            pl.BlockSpec((3, STEP, channels), lambda i: (0, i, 0)),
            whole((owners, atoms)),
        ),
        scratch_shapes=[
            pltpu.VMEM((owners * window, 5 * channels), bf16),
            pltpu.VMEM((STEP, 5 * channels), f32),
        ],
        compiler_params=pltpu.CompilerParams(dimension_semantics=("arbitrary",)),
        name="final",
    )(
        starts,
        rows,
        received,
        mixed,
        latent,
        scalar_proj,
        path_gain,
        energy_proj.reshape(1, latent_width),
    )
    sums = lax.all_to_all(sums, ("gy", "gz"), split_axis=0, concat_axis=0, tiled=True)
    return (latent_out, vector_out, jnp.sum(sums, axis=0))


def solution(mesh):
    placed = (
        P(("gx", "gy", "gz"), None),
        P(("gx", "gy", "gz"), None, None),
        P(("gx", "gy", "gz")),
        P(None, ("gx", "gy", "gz")),
        P(("gx", "gy", "gz")),
        P(("gx", "gy", "gz"), None),
        P(("gx", "gy", "gz")),
        P(("gx", "gy", "gz")),
        P(),
        P(),
        P(),
        P(),
        P(),
        P(),
        P(),
        P(),
    )

    return jax.shard_map(
        local,
        mesh=mesh,
        in_specs=placed,
        out_specs=(
            P(("gx", "gy", "gz"), None),
            P(None, ("gx", "gy", "gz"), None),
            P(("gx", "gy", "gz")),
        ),
        check_vma=False,
    )
```

```python
import functools

import jax
import jax.numpy as jnp
from jax import lax
from jax.experimental import pallas as pl
from jax.experimental.pallas import tpu as pltpu
from jax.sharding import PartitionSpec as P


cutoff = 6.0
root_two = 2.0**0.5
root_three = 3.0**0.5
root_five = 5.0**0.5
root_fifteen = 15.0**0.5
f32 = jnp.float32
bf16 = jnp.bfloat16
LANES = 128
STEP = 256
NT = (((1,), (1,)), ((), ()))


def silu(v):
    half = 0.5 * v
    return half + half * jnp.tanh(half)


def split3(v):
    high = v.astype(bf16).astype(f32)
    rest = v - high
    middle = rest.astype(bf16).astype(f32)
    return (high, middle, rest - middle)


def route_kernel(
    owners,
    cap,
    window,
    count_ref,
    owner_ref,
    center_ref,
    vec_ref,
    export_ref,
    rows_ref,
    starts_ref,
    request_ref,
):
    slots = owner_ref.shape[1]
    padded = request_ref.shape[2]
    owner = owner_ref[...]
    center = center_ref[...]
    member = owner == lax.broadcasted_iota(jnp.int32, (owners, slots), 0)
    member = jnp.where(member, 1.0, 0.0)
    step = STEP
    before = lax.broadcasted_iota(jnp.int32, (step, step), 0) < lax.broadcasted_iota(
        jnp.int32, (step, step), 1
    )
    before = jnp.where(before, 1.0, 0.0).astype(bf16)
    seen = jnp.zeros((owners, 1), f32)
    lane = lax.broadcasted_iota(jnp.int32, starts_ref.shape, 1)
    starts = jnp.zeros(starts_ref.shape, f32)
    ranks = []
    bases = []
    for start in range(0, slots, step):
        part = member[:, start : start + step]
        earlier = jnp.dot(part.astype(bf16), before, preferred_element_type=f32) + seen
        ranks.append(jnp.sum(part * earlier, axis=0, keepdims=True))
        base = jnp.minimum(jnp.floor(seen * (1.0 / 16.0)) * 16.0, cap - window)
        bases.append(jnp.sum(part * base, axis=0, keepdims=True))
        seen = seen + jnp.sum(part, axis=1, keepdims=True)
        starts = jnp.where(lane == start // step + 1, seen, starts)
    starts_ref[...] = starts.astype(jnp.int32)
    rank = jnp.concatenate(ranks, axis=1)
    place_in = owner.astype(f32) * window + rank - jnp.concatenate(bases, axis=1)
    position = lax.broadcasted_iota(jnp.int32, (1, slots), 1)
    live = jnp.where(position < count_ref[0], 1.0, 0.0)
    vec = vec_ref[...]
    length = jnp.sqrt(jnp.sum(vec * vec, axis=0, keepdims=True))
    unit = vec / jnp.maximum(length, 1.0)
    rows_ref[0:3, :] = root_three * unit
    rows_ref[3:4, :] = place_in
    rows_ref[4:5, :] = owner.astype(f32) * cap + rank
    rows_ref[5:6, :] = jnp.where(live > 0.5, owner.astype(f32), -1.0)
    rows_ref[6:7, :] = center.astype(f32)
    rows_ref[7:8, :] = length
    code = center + 1
    values = [(code // 256).astype(f32), (code % 256).astype(f32)]
    for m in range(3):
        values.extend(split3(vec[m : m + 1, :]))
    listed = member * live
    left = jnp.concatenate([(listed * v).astype(bf16) for v in values], axis=0)
    place = rank.astype(jnp.int32) == lax.broadcasted_iota(jnp.int32, (padded, slots), 0)
    place = jnp.where(place, 1.0, 0.0).astype(bf16)
    sent = lax.dot_general(left, place, NT, preferred_element_type=f32)
    at = lambda i: sent[i * owners : (i + 1) * owners, :]
    fields = [256.0 * at(0) + at(1)]
    fields += [at(2 + 3 * m) + at(3 + 3 * m) + at(4 + 3 * m) for m in range(3)]
    exports = export_ref.shape[1]
    exported = export_ref[...].astype(f32)
    free = padded - cap
    if request_ref.shape[1] == 4:
        lane = lax.broadcasted_iota(jnp.int32, (1, padded), 1)
        rest = jnp.concatenate([exported] * (-(-padded // exports)), axis=1)[:, :padded]
        for m in range(4):
            shift = (cap - m * free) % exports
            turned = pltpu.roll(jnp.broadcast_to(rest, (8, padded)), shift, 1)[:1]
            fields[m] = jnp.where(lane >= cap, turned, fields[m])
    for m in range(4):
        request_ref[:, m, :] = fields[m]
    for m in range(4, request_ref.shape[1]):
        piece = exported[:, (m - 4) * padded : (m - 3) * padded]
        request_ref[:, m, :] = jnp.broadcast_to(piece, (owners, padded))


def owner_kernel(cap, request_ref, env_ref, out_ref, table_ref):
    group = request_ref.shape[0]
    components, atoms, channels = env_ref.shape

    @pl.when(pl.program_id(0) == 0)
    def _():
        for m in range(components):
            table_ref[:, m * channels : (m + 1) * channels] = env_ref[m]

    masks = []
    weights = []
    for g in range(group):
        block = request_ref[g]
        code, vec = (block[0:1, :], block[1:4, :])
        length = jnp.sqrt(jnp.sum(vec * vec, axis=0, keepdims=True))
        unit = vec / jnp.maximum(length, 1.0)
        ux, uy, uz = (unit[0:1], unit[1:2], unit[2:3])
        rows = jnp.concatenate(
            [
                code,
                root_fifteen * ux * uy,
                root_fifteen * uy * uz,
                0.5 * root_five * (2.0 * uz * uz - ux * ux - uy * uy),
                root_fifteen * ux * uz,
                0.5 * root_fifteen * (ux * ux - uy * uy),
                jnp.zeros_like(code),
                jnp.zeros_like(code),
            ],
            axis=0,
        )
        columns = jnp.transpose(rows)[:cap]
        atom = lax.broadcasted_iota(jnp.int32, (cap, atoms), 1) + 1
        hit = columns[:, 0:1].astype(jnp.int32) == atom
        masks.append(jnp.where(hit, 1.0, 0.0).astype(bf16))
        weights.append(columns)
    pick = jnp.concatenate(masks, axis=0)
    weight = jnp.concatenate(weights, axis=0)
    found = jnp.dot(pick, table_ref[...], preferred_element_type=f32)
    keep = 4 * channels
    out_ref[:, :keep] = found[:, :keep].astype(bf16)
    total = weight[:, 1:2] * found[:, keep : keep + channels]
    for m in range(1, 5):
        start = keep + m * channels
        total = total + weight[:, 1 + m : 2 + m] * found[:, start : start + channels]
    out_ref[:, keep:] = total.astype(bf16)


def latent_kernel(basis, index_ref, lists_ref, rows_ref, *refs):
    pieces = refs[:-8]
    both_ref, radial_ref, hidden_ref, split_ref, latent_ref, mixed_ref = refs[-8:-2]
    table_ref, feat_ref = refs[-2:]
    many, _ = feat_ref.shape[1:]

    @pl.when(pl.program_id(0) == 0)
    def _():
        at = 0
        for piece in pieces:
            table_ref[at : at + piece.shape[0], :] = piece[...].astype(f32)
            at += piece.shape[0]

    start = pl.program_id(0) * many
    unroll = 16

    def gather(i, carry):
        at = pl.multiple_of(i * unroll, unroll)
        read = (start + at) * 3
        centers = [index_ref[read + 3 * j] for j in range(unroll)]
        entries = [index_ref[read + 3 * j + 2] for j in range(unroll)]
        neighbours = [index_ref[read + 3 * j + 1] + lists_ref[entries[j]] for j in range(unroll)]
        for j in range(unroll):
            feat_ref[0, pl.ds(at + j, 1), :] = table_ref[pl.ds(centers[j], 1), :]
            feat_ref[1, pl.ds(at + j, 1), :] = table_ref[pl.ds(neighbours[j], 1), :]
        return carry

    lax.fori_loop(0, many // unroll, gather, 0)
    spacing = cutoff / (basis - 1)
    length = rows_ref[7:8, :]
    centres = lax.broadcasted_iota(jnp.int32, (basis, many), 0).astype(f32) * spacing
    scaled = (length - centres) / spacing
    radial = jnp.concatenate(split3(jnp.exp(-(scaled * scaled))), axis=0)
    radial = jnp.transpose(radial).astype(bf16)
    feat = jnp.concatenate([feat_ref[0], feat_ref[1]], axis=1).astype(bf16)
    before = jnp.dot(feat, both_ref[...], preferred_element_type=f32)
    before = before + jnp.dot(radial, radial_ref[...], preferred_element_type=f32)
    hidden = silu(before).astype(bf16)
    after = jnp.dot(hidden, hidden_ref[...], preferred_element_type=f32)
    latent = silu(after).astype(bf16)
    latent_ref[...] = latent
    mixed_ref[...] = jnp.dot(latent, split_ref[...], preferred_element_type=f32)


def final_kernel(
    owners,
    cap,
    window,
    starts_ref,
    rows_ref,
    env_ref,
    mixed_ref,
    latent_ref,
    scalar_ref,
    gain_ref,
    energy_ref,
    latent_out_ref,
    vector_out_ref,
    sums_ref,
    near_ref,
    found_ref,
    total_ref,
):
    many = rows_ref.shape[1]
    places = env_ref.shape[0]
    channels = gain_ref.shape[1]
    atoms = sums_ref.shape[1]
    columns = jnp.transpose(rows_ref[...])

    def pick(part, column, size):
        wanted = columns[part * STEP : (part + 1) * STEP, column : column + 1]
        hit = wanted.astype(jnp.int32) == lax.broadcasted_iota(jnp.int32, (STEP, size), 1)
        return jnp.where(hit, 1.0, 0.0).astype(bf16)

    def find(part):
        step = pl.program_id(0) * (many // STEP) + part
        here = pl.ds(part * STEP, STEP)
        fits = True
        bases = []
        for o in range(owners):
            base = jnp.minimum(starts_ref[o, step] // 16 * 16, cap - window)
            bases.append(base)
            fits = fits & (starts_ref[o, step + 1] <= base + window)

        @pl.when(fits)
        def _():
            for o in range(owners):
                at = pl.multiple_of(o * cap + bases[o], 16)
                near_ref[o * window : (o + 1) * window, :] = env_ref[pl.ds(at, window), :]
            found_ref[here, :] = jnp.dot(
                pick(part, 3, owners * window), near_ref[...], preferred_element_type=f32
            )

        @pl.when(jnp.logical_not(fits))
        def _():
            found_ref[here, :] = jnp.dot(
                pick(part, 4, places), env_ref[...], preferred_element_type=f32
            )

    for part in range(many // STEP):
        find(part)

    env = found_ref[...]
    part = lambda i: env[:, i * channels : (i + 1) * channels]
    env_scalar, env_vector, tensor = (part(0), [part(1), part(2), part(3)], part(4))
    mixed = mixed_ref[...]
    scalar_part = mixed[:, :channels]
    vector_part = mixed[:, channels : 2 * channels]
    tensor_part = mixed[:, 2 * channels :]
    edge = [vector_part * columns[:, m : m + 1] for m in range(3)]
    vector_dot = edge[0] * env_vector[0] + edge[1] * env_vector[1] + edge[2] * env_vector[2]
    invariants = jnp.concatenate(
        [
            (scalar_part * env_scalar).astype(bf16),
            (vector_dot * (1.0 / root_three)).astype(bf16),
            (tensor_part * tensor * (1.0 / root_five)).astype(bf16),
        ],
        axis=1,
    )
    live = columns[:, 5:6] >= 0.0
    cross = [
        edge[1] * env_vector[2] - edge[2] * env_vector[1],
        edge[2] * env_vector[0] - edge[0] * env_vector[2],
        edge[0] * env_vector[1] - edge[1] * env_vector[0],
    ]
    gain = gain_ref[...]
    for m in range(3):
        value = (
            gain[0:1] * scalar_part * env_vector[m]
            + gain[1:2] * edge[m] * env_scalar
            + (gain[2:3] * (1.0 / root_two)) * cross[m]
        )
        vector_out_ref[m] = jnp.where(live, value, 0.0).astype(bf16)
    update = jnp.dot(invariants, scalar_ref[...], preferred_element_type=f32)
    update = silu(update)
    latent = jnp.where(live, latent_ref[...].astype(f32) + update, 0.0).astype(bf16)
    latent_out_ref[...] = latent
    energy = jnp.sum(latent.astype(f32) * energy_ref[...], axis=1, keepdims=True)
    lane = lax.broadcasted_iota(jnp.int32, (many, LANES), 1)
    owner = columns[:, 5:6].astype(jnp.int32)
    spread = jnp.zeros((many, LANES), f32)
    for i, piece in enumerate(split3(energy)):
        spread = spread + jnp.where(lane == owner + i * owners, piece, 0.0)
    center = rows_ref[6:7, :].astype(jnp.int32)
    of_atom = center == lax.broadcasted_iota(jnp.int32, (atoms, many), 0)
    of_atom = jnp.where(of_atom, 1.0, 0.0).astype(bf16)
    sums = jnp.dot(of_atom, spread.astype(bf16), preferred_element_type=f32)

    @pl.when(pl.program_id(0) == 0)
    def _():
        total_ref[...] = sums

    @pl.when(pl.program_id(0) > 0)
    def _():
        total_ref[...] = total_ref[...] + sums

    @pl.when(pl.program_id(0) == pl.num_programs(0) - 1)
    def _():
        total = jnp.transpose(total_ref[...])
        sums_ref[...] = sum(total[i * owners : (i + 1) * owners] for i in range(3))


def whole(shape):
    return pl.BlockSpec(shape, lambda *_: (0,) * len(shape))


def swap(x, axis, bit):
    return lax.ppermute(x, axis, [(i, i ^ bit) for i in range(lax.axis_size(axis))])


def across(pieces, size):
    bit = size // 2
    while bit:
        for (y, z), piece in list(pieces.items()):
            pieces[y ^ bit, z] = swap(piece, "gy", bit)
        bit //= 2


def local(
    atom_feat,
    atom_env,
    export_index,
    pair_vec,
    pair_center,
    pair_owner,
    pair_neigh,
    pair_count,
    center_proj,
    neighbour_proj,
    radial_proj,
    hidden_proj,
    split_proj,
    scalar_proj,
    path_gain,
    energy_proj,
):
    atoms, channels = atom_feat.shape
    slots = pair_center.shape[0]
    exports = export_index.shape[0]
    latent_width = hidden_proj.shape[1]
    nx, ny, nz = (lax.axis_size("gx"), lax.axis_size("gy"), lax.axis_size("gz"))
    owners = ny * nz
    cap = 3 * slots // (2 * owners)
    padded = -(-cap // LANES) * LANES
    components = atom_env.shape[1]

    fields = 4 if 4 * (padded - cap) >= exports else 4 + -(-exports // padded)
    window = min(64, cap)
    rows, starts, request = pl.pallas_call(
        functools.partial(route_kernel, owners, cap, window),
        out_shape=(
            jax.ShapeDtypeStruct((8, slots), f32),
            jax.ShapeDtypeStruct((owners, LANES), jnp.int32),
            jax.ShapeDtypeStruct((owners, fields, padded), f32),
        ),
        in_specs=[pl.BlockSpec(memory_space=pltpu.SMEM)]
        + [pl.BlockSpec(memory_space=pltpu.VMEM)] * 4,
        out_specs=[pl.BlockSpec(memory_space=pltpu.VMEM)] * 3,
        name="route",
    )(
        pair_count,
        pair_owner.reshape(1, slots),
        pair_center.reshape(1, slots),
        pair_vec,
        export_index.reshape(1, exports),
    )
    request = lax.all_to_all(request, ("gy", "gz"), split_axis=0, concat_axis=0, tiled=True)

    my_y, my_z = (lax.axis_index("gy"), lax.axis_index("gz"))
    feat, request = lax.optimization_barrier((atom_feat, request))
    feats = {(0, 0): feat}
    for k in range(1, nz):
        feats[0, k] = swap(feat, "gz", k)
    across(feats, ny)

    group = min(4, owners)
    env = jnp.transpose(atom_env, (1, 0, 2))
    sent = pl.pallas_call(
        functools.partial(owner_kernel, cap),
        grid=(owners // group,),
        out_shape=jax.ShapeDtypeStruct((owners * cap, 5 * channels), bf16),
        in_specs=[
            pl.BlockSpec((group, fields, padded), lambda i: (i, 0, 0)),
            whole((components, atoms, channels)),
        ],
        out_specs=pl.BlockSpec((group * cap, 5 * channels), lambda i: (i, 0)),
        scratch_shapes=[pltpu.VMEM((atoms, components * channels), bf16)],
        compiler_params=pltpu.CompilerParams(dimension_semantics=("arbitrary",)),
        cost_estimate=pl.CostEstimate(
            flops=2 * owners * cap * atoms * components * channels,
            bytes_accessed=8 * atoms * components * channels,
            transcendentals=0,
        ),
        name="owner",
    )(request, env)
    if fields == 4:
        lists = request[:, :, cap:].reshape(owners, -1)[:, :exports]
    else:
        lists = request[:, 4:, :].reshape(owners, -1)[:, :exports]
    lists, sent = lax.optimization_barrier((lists, sent))
    received = lax.all_to_all(
        sent.reshape(owners, cap, 5 * channels),
        ("gy", "gz"),
        split_axis=0,
        concat_axis=0,
        tiled=True,
    ).reshape(owners * cap, 5 * channels)

    lists = lists.astype(jnp.int32)
    along = lax.dynamic_index_in_dim(lists.reshape(ny, nz, exports), my_y, 0, keepdims=False)
    along = along[jnp.arange(nz) ^ my_z] + jnp.arange(nz)[:, None] * atoms
    column = jnp.concatenate([feats[0, k] for k in range(nz)], axis=0)
    exported = column[along.reshape(-1)]
    up = [(i, (i + 1) % nx) for i in range(nx)]
    down = [(j, i) for i, j in up]
    beyond = [lax.ppermute(exported, "gx", up)]
    if nx > 2:
        beyond.append(lax.ppermute(exported, "gx", down))
    beyond = jnp.concatenate(beyond, axis=0)

    owner = pair_owner[:, 0]
    oy, oz = (owner // nz, owner % nz)

    def cell_of(y, z):
        return (y ^ my_y) * nz + (z ^ my_z)

    k = jnp.maximum(pair_neigh - atoms, 0)
    cell, member = (k // exports, k % exports)
    dx, dy, dz = (cell // 9 - 1, cell // 3 % 3 - 1, cell % 3 - 1)
    sy, sz = ((oy + dy) % ny, (oz + dz) % nz)
    sides = beyond.shape[0] // (nz * exports)
    outside = (sy ^ my_y) * sides
    if nx > 2:
        outside = outside + jnp.where(dx < 0, 0, 1)
    outside = owners * atoms + (outside * nz + (sz ^ my_z)) * exports + member
    home = cell_of(oy, oz) * atoms
    own = pair_neigh < atoms
    listed = (pair_neigh >= atoms) & (dx == 0)
    halo_at = jnp.where(dx == 0, cell_of(sy, sz) * atoms, outside)
    entry = jnp.where(listed, (sy * nz + sz) * exports + member + 1, 0)
    lists = jnp.concatenate([jnp.zeros((1,), jnp.int32), lists.reshape(-1)])
    neighbour_at = jnp.where(own, home + pair_neigh, halo_at)
    index = jnp.stack([home + pair_center, neighbour_at, entry], axis=1).reshape(-1)
    beyond, index, lists = lax.optimization_barrier((beyond, index, lists))
    edges = {(0, 0): beyond}
    across(edges, ny)
    pieces = [feats[i // nz, i % nz] for i in range(owners)] + [edges[i, 0] for i in range(ny)]
    table_rows = sum(piece.shape[0] for piece in pieces)
    many = min(512, slots)
    basis = radial_proj.shape[0]
    latent, mixed = pl.pallas_call(
        functools.partial(latent_kernel, basis),
        grid=(slots // many,),
        out_shape=(
            jax.ShapeDtypeStruct((slots, latent_width), bf16),
            jax.ShapeDtypeStruct((slots, 3 * channels), f32),
        ),
        in_specs=[
            pl.BlockSpec(memory_space=pltpu.SMEM),
            pl.BlockSpec(memory_space=pltpu.SMEM),
            pl.BlockSpec((8, many), lambda i: (0, i)),
        ]
        + [pl.BlockSpec(memory_space=pltpu.VMEM)] * (len(pieces) + 4),
        out_specs=(
            pl.BlockSpec((many, latent_width), lambda i: (i, 0)),
            pl.BlockSpec((many, 3 * channels), lambda i: (i, 0)),
        ),
        scratch_shapes=[
            pltpu.VMEM((table_rows, channels), f32),
            pltpu.VMEM((2, many, channels), f32),
        ],
        compiler_params=pltpu.CompilerParams(dimension_semantics=("arbitrary",)),
        cost_estimate=pl.CostEstimate(
            flops=2 * slots * latent_width * (2 * latent_width + 3 * channels),
            bytes_accessed=2 * table_rows * channels,
            transcendentals=4 * slots * latent_width,
        ),
        name="latent",
    )(
        index,
        lists,
        rows,
        *pieces,
        jnp.concatenate([center_proj, neighbour_proj], axis=0),
        jnp.concatenate([radial_proj] * 3, axis=0),
        hidden_proj,
        split_proj,
    )

    latent_out, vector_out, sums = pl.pallas_call(
        functools.partial(final_kernel, owners, cap, window),
        grid=(slots // many,),
        out_shape=(
            jax.ShapeDtypeStruct((slots, latent_width), bf16),
            jax.ShapeDtypeStruct((3, slots, channels), bf16),
            jax.ShapeDtypeStruct((owners, atoms), f32),
        ),
        in_specs=[
            pl.BlockSpec(memory_space=pltpu.SMEM),
            pl.BlockSpec((8, many), lambda i: (0, i)),
            whole((owners * cap, 5 * channels)),
            pl.BlockSpec((many, 3 * channels), lambda i: (i, 0)),
            pl.BlockSpec((many, latent_width), lambda i: (i, 0)),
            whole(scalar_proj.shape),
            whole(path_gain.shape),
            whole((1, latent_width)),
        ],
        out_specs=(
            pl.BlockSpec((many, latent_width), lambda i: (i, 0)),
            pl.BlockSpec((3, many, channels), lambda i: (0, i, 0)),
            whole((owners, atoms)),
        ),
        scratch_shapes=[
            pltpu.VMEM((owners * window, 5 * channels), bf16),
            pltpu.VMEM((many, 5 * channels), f32),
            pltpu.VMEM((atoms, LANES), f32),
        ],
        compiler_params=pltpu.CompilerParams(dimension_semantics=("arbitrary",)),
        name="final",
    )(
        starts,
        rows,
        received,
        mixed,
        latent,
        scalar_proj,
        path_gain,
        energy_proj.reshape(1, latent_width),
    )
    sums = lax.all_to_all(sums, ("gy", "gz"), split_axis=0, concat_axis=0, tiled=True)
    return (latent_out, vector_out, jnp.sum(sums, axis=0))


def solution(mesh):
    placed = (
        P(("gx", "gy", "gz"), None),
        P(("gx", "gy", "gz"), None, None),
        P(("gx", "gy", "gz")),
        P(None, ("gx", "gy", "gz")),
        P(("gx", "gy", "gz")),
        P(("gx", "gy", "gz"), None),
        P(("gx", "gy", "gz")),
        P(("gx", "gy", "gz")),
        P(),
        P(),
        P(),
        P(),
        P(),
        P(),
        P(),
        P(),
    )

    return jax.shard_map(
        local,
        mesh=mesh,
        in_specs=placed,
        out_specs=(
            P(("gx", "gy", "gz"), None),
            P(None, ("gx", "gy", "gz"), None),
            P(("gx", "gy", "gz")),
        ),
        check_vma=False,
    )
```

```python
import functools

import jax
import jax.numpy as jnp
from jax import lax
from jax.experimental import pallas as pl
from jax.experimental.pallas import tpu as pltpu
from jax.sharding import PartitionSpec as P


cutoff = 6.0
root_two = 2.0**0.5
root_three = 3.0**0.5
root_five = 5.0**0.5
root_fifteen = 15.0**0.5
f32 = jnp.float32
bf16 = jnp.bfloat16
LANES = 128
STEP = 256
NT = (((1,), (1,)), ((), ()))


def silu(v):
    half = 0.5 * v
    return half + half * jnp.tanh(half)


def split3(v):
    high = v.astype(bf16).astype(f32)
    rest = v - high
    middle = rest.astype(bf16).astype(f32)
    return (high, middle, rest - middle)


def route_kernel(
    owners,
    cap,
    window,
    count_ref,
    owner_ref,
    center_ref,
    vec_ref,
    export_ref,
    rows_ref,
    starts_ref,
    request_ref,
):
    slots = owner_ref.shape[1]
    padded = request_ref.shape[2]
    owner = owner_ref[...]
    center = center_ref[...]
    member = owner == lax.broadcasted_iota(jnp.int32, (owners, slots), 0)
    member = jnp.where(member, 1.0, 0.0)
    step = STEP
    before = lax.broadcasted_iota(jnp.int32, (step, step), 0) < lax.broadcasted_iota(
        jnp.int32, (step, step), 1
    )
    before = jnp.where(before, 1.0, 0.0).astype(bf16)
    seen = jnp.zeros((owners, 1), f32)
    lane = lax.broadcasted_iota(jnp.int32, (owners, LANES), 1)
    first = lax.broadcasted_iota(jnp.int32, (owners, LANES), 0).astype(f32) * cap
    offsets = jnp.zeros((owners, LANES), f32)
    most = jnp.zeros((1, LANES), f32)
    ranks = []
    bases = []
    for start in range(0, slots, step):
        part = member[:, start : start + step]
        earlier = jnp.dot(part.astype(bf16), before, preferred_element_type=f32) + seen
        ranks.append(jnp.sum(part * earlier, axis=0, keepdims=True))
        base = jnp.minimum(jnp.floor(seen * (1.0 / 16.0)) * 16.0, cap - window)
        bases.append(jnp.sum(part * base, axis=0, keepdims=True))
        seen = seen + jnp.sum(part, axis=1, keepdims=True)
        past = jnp.max(seen - base, axis=0, keepdims=True)
        offsets = jnp.where(lane == start // step, first + base, offsets)
        most = jnp.where(lane[:1] == start // step, past, most)
    starts_ref[:owners, :] = offsets.astype(jnp.int32)
    starts_ref[owners:, :] = jnp.broadcast_to(most, (8, LANES)).astype(jnp.int32)
    rank = jnp.concatenate(ranks, axis=1)
    place_in = owner.astype(f32) * window + rank - jnp.concatenate(bases, axis=1)
    position = lax.broadcasted_iota(jnp.int32, (1, slots), 1)
    live = jnp.where(position < count_ref[0], 1.0, 0.0)
    vec = vec_ref[...]
    length = jnp.sqrt(jnp.sum(vec * vec, axis=0, keepdims=True))
    unit = vec / jnp.maximum(length, 1.0)
    rows_ref[0:3, :] = root_three * unit
    rows_ref[3:4, :] = place_in
    rows_ref[4:5, :] = owner.astype(f32) * cap + rank
    rows_ref[5:6, :] = jnp.where(live > 0.5, owner.astype(f32), -1.0)
    rows_ref[6:7, :] = center.astype(f32)
    rows_ref[7:8, :] = length
    code = center + 1
    values = [(code // 256).astype(f32), (code % 256).astype(f32)]
    for m in range(3):
        values.extend(split3(vec[m : m + 1, :]))
    listed = member * live
    left = jnp.concatenate([(listed * v).astype(bf16) for v in values], axis=0)
    place = rank.astype(jnp.int32) == lax.broadcasted_iota(jnp.int32, (padded, slots), 0)
    place = jnp.where(place, 1.0, 0.0).astype(bf16)
    sent = lax.dot_general(left, place, NT, preferred_element_type=f32)
    at = lambda i: sent[i * owners : (i + 1) * owners, :]
    fields = [256.0 * at(0) + at(1)]
    fields += [at(2 + 3 * m) + at(3 + 3 * m) + at(4 + 3 * m) for m in range(3)]
    exports = export_ref.shape[1]
    exported = export_ref[...].astype(f32)
    free = padded - cap
    if request_ref.shape[1] == 4:
        lane = lax.broadcasted_iota(jnp.int32, (1, padded), 1)
        rest = jnp.concatenate([exported] * (-(-padded // exports)), axis=1)[:, :padded]
        for m in range(4):
            shift = (cap - m * free) % exports
            turned = pltpu.roll(jnp.broadcast_to(rest, (8, padded)), shift, 1)[:1]
            fields[m] = jnp.where(lane >= cap, turned, fields[m])
    for m in range(4):
        request_ref[:, m, :] = fields[m]
    for m in range(4, request_ref.shape[1]):
        piece = exported[:, (m - 4) * padded : (m - 3) * padded]
        request_ref[:, m, :] = jnp.broadcast_to(piece, (owners, padded))


def owner_kernel(cap, request_ref, env_ref, out_ref, table_ref):
    group = request_ref.shape[0]
    components, atoms, channels = env_ref.shape

    @pl.when(pl.program_id(0) == 0)
    def _():
        for m in range(components):
            table_ref[:, m * channels : (m + 1) * channels] = env_ref[m]

    masks = []
    weights = []
    for g in range(group):
        block = request_ref[g]
        code, vec = (block[0:1, :], block[1:4, :])
        length = jnp.sqrt(jnp.sum(vec * vec, axis=0, keepdims=True))
        unit = vec / jnp.maximum(length, 1.0)
        ux, uy, uz = (unit[0:1], unit[1:2], unit[2:3])
        rows = jnp.concatenate(
            [
                code,
                root_fifteen * ux * uy,
                root_fifteen * uy * uz,
                0.5 * root_five * (2.0 * uz * uz - ux * ux - uy * uy),
                root_fifteen * ux * uz,
                0.5 * root_fifteen * (ux * ux - uy * uy),
                jnp.zeros_like(code),
                jnp.zeros_like(code),
            ],
            axis=0,
        )
        columns = jnp.transpose(rows)[:cap]
        atom = lax.broadcasted_iota(jnp.int32, (cap, atoms), 1) + 1
        hit = columns[:, 0:1].astype(jnp.int32) == atom
        masks.append(jnp.where(hit, 1.0, 0.0).astype(bf16))
        weights.append(columns)
    pick = jnp.concatenate(masks, axis=0)
    weight = jnp.concatenate(weights, axis=0)
    found = jnp.dot(pick, table_ref[...], preferred_element_type=f32)
    keep = 4 * channels
    out_ref[:, :keep] = found[:, :keep].astype(bf16)
    total = weight[:, 1:2] * found[:, keep : keep + channels]
    for m in range(1, 5):
        start = keep + m * channels
        total = total + weight[:, 1 + m : 2 + m] * found[:, start : start + channels]
    out_ref[:, keep:] = total.astype(bf16)


def latent_kernel(basis, index_ref, lists_ref, rows_ref, *refs):
    pieces = refs[:-8]
    both_ref, radial_ref, hidden_ref, split_ref, latent_ref, mixed_ref = refs[-8:-2]
    table_ref, feat_ref = refs[-2:]
    many, _ = feat_ref.shape[1:]

    @pl.when(pl.program_id(0) == 0)
    def _():
        at = 0
        for piece in pieces:
            table_ref[at : at + piece.shape[0], :] = piece[...].astype(f32)
            at += piece.shape[0]

    start = pl.program_id(0) * many
    unroll = 16

    def gather(i, carry):
        at = pl.multiple_of(i * unroll, unroll)
        read = (start + at) * 3
        centers = [index_ref[read + 3 * j] for j in range(unroll)]
        entries = [index_ref[read + 3 * j + 2] for j in range(unroll)]
        neighbours = [index_ref[read + 3 * j + 1] + lists_ref[entries[j]] for j in range(unroll)]
        for j in range(unroll):
            feat_ref[0, pl.ds(at + j, 1), :] = table_ref[pl.ds(centers[j], 1), :]
            feat_ref[1, pl.ds(at + j, 1), :] = table_ref[pl.ds(neighbours[j], 1), :]
        return carry

    lax.fori_loop(0, many // unroll, gather, 0)
    spacing = cutoff / (basis - 1)
    length = rows_ref[7:8, :]
    centres = lax.broadcasted_iota(jnp.int32, (basis, many), 0).astype(f32) * spacing
    scaled = (length - centres) / spacing
    radial = jnp.concatenate(split3(jnp.exp(-(scaled * scaled))), axis=0)
    radial = jnp.transpose(radial).astype(bf16)
    feat = jnp.concatenate([feat_ref[0], feat_ref[1]], axis=1).astype(bf16)
    before = jnp.dot(feat, both_ref[...], preferred_element_type=f32)
    before = before + jnp.dot(radial, radial_ref[...], preferred_element_type=f32)
    hidden = silu(before).astype(bf16)
    after = jnp.dot(hidden, hidden_ref[...], preferred_element_type=f32)
    latent = silu(after).astype(bf16)
    latent_ref[...] = latent
    mixed_ref[...] = jnp.dot(latent, split_ref[...], preferred_element_type=f32)


def final_kernel(
    owners,
    window,
    starts_ref,
    rows_ref,
    env_ref,
    mixed_ref,
    latent_ref,
    scalar_ref,
    gain_ref,
    energy_ref,
    latent_out_ref,
    vector_out_ref,
    sums_ref,
    near_ref,
    found_ref,
    total_ref,
):
    many = rows_ref.shape[1]
    places = env_ref.shape[0]
    channels = gain_ref.shape[1]
    atoms = sums_ref.shape[1] * LANES
    columns = jnp.transpose(rows_ref[...])

    def pick(part, column, size):
        wanted = columns[part * STEP : (part + 1) * STEP, column : column + 1]
        hit = wanted.astype(jnp.int32) == lax.broadcasted_iota(jnp.int32, (STEP, size), 1)
        return jnp.where(hit, 1.0, 0.0).astype(bf16)

    def find(part):
        step = pl.program_id(0) * (many // STEP) + part
        here = pl.ds(part * STEP, STEP)
        fits = starts_ref[owners, step] <= window

        @pl.when(fits)
        def _():
            for o in range(owners):
                at = pl.multiple_of(starts_ref[o, step], 16)
                near_ref[o * window : (o + 1) * window, :] = env_ref[pl.ds(at, window), :]
            found_ref[here, :] = jnp.dot(
                pick(part, 3, owners * window), near_ref[...], preferred_element_type=f32
            )

        @pl.when(jnp.logical_not(fits))
        def _():
            found_ref[here, :] = jnp.dot(
                pick(part, 4, places), env_ref[...], preferred_element_type=f32
            )

    for part in range(many // STEP):
        find(part)

    env = found_ref[...]
    part = lambda i: env[:, i * channels : (i + 1) * channels]
    env_scalar, env_vector, tensor = (part(0), [part(1), part(2), part(3)], part(4))
    mixed = mixed_ref[...]
    scalar_part = mixed[:, :channels]
    vector_part = mixed[:, channels : 2 * channels]
    tensor_part = mixed[:, 2 * channels :]
    edge = [vector_part * columns[:, m : m + 1] for m in range(3)]
    vector_dot = edge[0] * env_vector[0] + edge[1] * env_vector[1] + edge[2] * env_vector[2]
    invariants = jnp.concatenate(
        [
            (scalar_part * env_scalar).astype(bf16),
            (vector_dot * (1.0 / root_three)).astype(bf16),
            (tensor_part * tensor * (1.0 / root_five)).astype(bf16),
        ],
        axis=1,
    )
    live = columns[:, 5:6] >= 0.0
    cross = [
        edge[1] * env_vector[2] - edge[2] * env_vector[1],
        edge[2] * env_vector[0] - edge[0] * env_vector[2],
        edge[0] * env_vector[1] - edge[1] * env_vector[0],
    ]
    gain = gain_ref[...]
    for m in range(3):
        value = (
            gain[0:1] * scalar_part * env_vector[m]
            + gain[1:2] * edge[m] * env_scalar
            + (gain[2:3] * (1.0 / root_two)) * cross[m]
        )
        vector_out_ref[m] = jnp.where(live, value, 0.0).astype(bf16)
    update = jnp.dot(invariants, scalar_ref[...], preferred_element_type=f32)
    update = silu(update)
    latent = jnp.where(live, latent_ref[...].astype(f32) + update, 0.0).astype(bf16)
    latent_out_ref[...] = latent
    energy = jnp.sum(latent.astype(f32) * energy_ref[...], axis=1, keepdims=True)
    lane = lax.broadcasted_iota(jnp.int32, (many, LANES), 1)
    owner = columns[:, 5:6].astype(jnp.int32)
    spread = jnp.zeros((many, LANES), f32)
    for i, piece in enumerate(split3(energy)):
        spread = spread + jnp.where(lane == owner + i * owners, piece, 0.0)
    center = rows_ref[6:7, :].astype(jnp.int32)
    of_atom = center == lax.broadcasted_iota(jnp.int32, (atoms, many), 0)
    of_atom = jnp.where(of_atom, 1.0, 0.0).astype(bf16)
    sums = jnp.dot(of_atom, spread.astype(bf16), preferred_element_type=f32)

    @pl.when(pl.program_id(0) == 0)
    def _():
        total_ref[...] = sums

    @pl.when(pl.program_id(0) > 0)
    def _():
        total_ref[...] = total_ref[...] + sums

    @pl.when(pl.program_id(0) == pl.num_programs(0) - 1)
    def _():
        total = jnp.transpose(total_ref[...])
        total = sum(total[i * owners : (i + 1) * owners] for i in range(3))
        for i in range(atoms // LANES):
            sums_ref[:, i, :] = total[:, i * LANES : (i + 1) * LANES]


def whole(shape):
    return pl.BlockSpec(shape, lambda *_: (0,) * len(shape))


def swap(x, axis, bit):
    return lax.ppermute(x, axis, [(i, i ^ bit) for i in range(lax.axis_size(axis))])


def across(pieces, size):
    bit = size // 2
    while bit:
        for (y, z), piece in list(pieces.items()):
            pieces[y ^ bit, z] = swap(piece, "gy", bit)
        bit //= 2


def local(
    atom_feat,
    atom_env,
    export_index,
    pair_vec,
    pair_center,
    pair_owner,
    pair_neigh,
    pair_count,
    center_proj,
    neighbour_proj,
    radial_proj,
    hidden_proj,
    split_proj,
    scalar_proj,
    path_gain,
    energy_proj,
):
    atoms, channels = atom_feat.shape
    slots = pair_center.shape[0]
    exports = export_index.shape[0]
    latent_width = hidden_proj.shape[1]
    nx, ny, nz = (lax.axis_size("gx"), lax.axis_size("gy"), lax.axis_size("gz"))
    owners = ny * nz
    cap = 3 * slots // (2 * owners)
    padded = -(-cap // LANES) * LANES
    components = atom_env.shape[1]

    fields = 4 if 4 * (padded - cap) >= exports else 4 + -(-exports // padded)
    window = min(48, cap)
    rows, starts, request = pl.pallas_call(
        functools.partial(route_kernel, owners, cap, window),
        out_shape=(
            jax.ShapeDtypeStruct((8, slots), f32),
            jax.ShapeDtypeStruct((owners + 8, LANES), jnp.int32),
            jax.ShapeDtypeStruct((owners, fields, padded), f32),
        ),
        in_specs=[pl.BlockSpec(memory_space=pltpu.SMEM)]
        + [pl.BlockSpec(memory_space=pltpu.VMEM)] * 4,
        out_specs=[pl.BlockSpec(memory_space=pltpu.VMEM)] * 3,
        name="route",
    )(
        pair_count,
        pair_owner.reshape(1, slots),
        pair_center.reshape(1, slots),
        pair_vec,
        export_index.reshape(1, exports),
    )
    request = lax.all_to_all(request, ("gy", "gz"), split_axis=0, concat_axis=0, tiled=True)

    my_y, my_z = (lax.axis_index("gy"), lax.axis_index("gz"))
    feat, request = lax.optimization_barrier((atom_feat, request))
    feats = {(0, 0): feat}
    for k in range(1, nz):
        feats[0, k] = swap(feat, "gz", k)
    across(feats, ny)

    group = min(8, owners)
    env = jnp.transpose(atom_env, (1, 0, 2))
    sent = pl.pallas_call(
        functools.partial(owner_kernel, cap),
        grid=(owners // group,),
        out_shape=jax.ShapeDtypeStruct((owners * cap, 5 * channels), bf16),
        in_specs=[
            pl.BlockSpec((group, fields, padded), lambda i: (i, 0, 0)),
            whole((components, atoms, channels)),
        ],
        out_specs=pl.BlockSpec((group * cap, 5 * channels), lambda i: (i, 0)),
        scratch_shapes=[pltpu.VMEM((atoms, components * channels), bf16)],
        compiler_params=pltpu.CompilerParams(dimension_semantics=("arbitrary",)),
        cost_estimate=pl.CostEstimate(
            flops=2 * owners * cap * atoms * components * channels,
            bytes_accessed=8 * atoms * components * channels,
            transcendentals=0,
        ),
        name="owner",
    )(request, env)
    if fields == 4:
        lists = request[:, :, cap:].reshape(owners, -1)[:, :exports]
    else:
        lists = request[:, 4:, :].reshape(owners, -1)[:, :exports]
    lists, sent = lax.optimization_barrier((lists, sent))
    received = lax.all_to_all(
        sent.reshape(owners, cap, 5 * channels),
        ("gy", "gz"),
        split_axis=0,
        concat_axis=0,
        tiled=True,
    ).reshape(owners * cap, 5 * channels)

    lists = lists.astype(jnp.int32)
    along = lax.dynamic_index_in_dim(lists.reshape(ny, nz, exports), my_y, 0, keepdims=False)
    along = along[jnp.arange(nz) ^ my_z] + jnp.arange(nz)[:, None] * atoms
    column = jnp.concatenate([feats[0, k] for k in range(nz)], axis=0)
    exported = column[along.reshape(-1)]
    up = [(i, (i + 1) % nx) for i in range(nx)]
    down = [(j, i) for i, j in up]
    beyond = [lax.ppermute(exported, "gx", up)]
    if nx > 2:
        beyond.append(lax.ppermute(exported, "gx", down))
    beyond = jnp.concatenate(beyond, axis=0)

    owner = pair_owner[:, 0]
    oy, oz = (owner // nz, owner % nz)

    def cell_of(y, z):
        return (y ^ my_y) * nz + (z ^ my_z)

    k = jnp.maximum(pair_neigh - atoms, 0)
    cell, member = (k // exports, k % exports)
    dx, dy, dz = (cell // 9 - 1, cell // 3 % 3 - 1, cell % 3 - 1)
    sy, sz = ((oy + dy) % ny, (oz + dz) % nz)
    sides = beyond.shape[0] // (nz * exports)
    outside = (sy ^ my_y) * sides
    if nx > 2:
        outside = outside + jnp.where(dx < 0, 0, 1)
    outside = owners * atoms + (outside * nz + (sz ^ my_z)) * exports + member
    home = cell_of(oy, oz) * atoms
    own = pair_neigh < atoms
    listed = (pair_neigh >= atoms) & (dx == 0)
    halo_at = jnp.where(dx == 0, cell_of(sy, sz) * atoms, outside)
    entry = jnp.where(listed, (sy * nz + sz) * exports + member + 1, 0)
    lists = jnp.concatenate([jnp.zeros((1,), jnp.int32), lists.reshape(-1)])
    neighbour_at = jnp.where(own, home + pair_neigh, halo_at)
    index = jnp.stack([home + pair_center, neighbour_at, entry], axis=1).reshape(-1)
    beyond, index, lists = lax.optimization_barrier((beyond, index, lists))
    edges = {(0, 0): beyond}
    across(edges, ny)
    pieces = [feats[i // nz, i % nz] for i in range(owners)] + [edges[i, 0] for i in range(ny)]
    table_rows = sum(piece.shape[0] for piece in pieces)
    many = min(512, slots)
    basis = radial_proj.shape[0]
    latent, mixed = pl.pallas_call(
        functools.partial(latent_kernel, basis),
        grid=(slots // many,),
        out_shape=(
            jax.ShapeDtypeStruct((slots, latent_width), bf16),
            jax.ShapeDtypeStruct((slots, 3 * channels), f32),
        ),
        in_specs=[
            pl.BlockSpec(memory_space=pltpu.SMEM),
            pl.BlockSpec(memory_space=pltpu.SMEM),
            pl.BlockSpec((8, many), lambda i: (0, i)),
        ]
        + [pl.BlockSpec(memory_space=pltpu.VMEM)] * (len(pieces) + 4),
        out_specs=(
            pl.BlockSpec((many, latent_width), lambda i: (i, 0)),
            pl.BlockSpec((many, 3 * channels), lambda i: (i, 0)),
        ),
        scratch_shapes=[
            pltpu.VMEM((table_rows, channels), f32),
            pltpu.VMEM((2, many, channels), f32),
        ],
        compiler_params=pltpu.CompilerParams(dimension_semantics=("arbitrary",)),
        cost_estimate=pl.CostEstimate(
            flops=2 * slots * latent_width * (2 * latent_width + 3 * channels),
            bytes_accessed=2 * table_rows * channels,
            transcendentals=4 * slots * latent_width,
        ),
        name="latent",
    )(
        index,
        lists,
        rows,
        *pieces,
        jnp.concatenate([center_proj, neighbour_proj], axis=0),
        jnp.concatenate([radial_proj] * 3, axis=0),
        hidden_proj,
        split_proj,
    )

    latent_out, vector_out, sums = pl.pallas_call(
        functools.partial(final_kernel, owners, window),
        grid=(slots // many,),
        out_shape=(
            jax.ShapeDtypeStruct((slots, latent_width), bf16),
            jax.ShapeDtypeStruct((3, slots, channels), bf16),
            jax.ShapeDtypeStruct((owners, atoms // LANES, LANES), f32),
        ),
        in_specs=[
            pl.BlockSpec(memory_space=pltpu.SMEM),
            pl.BlockSpec((8, many), lambda i: (0, i)),
            whole((owners * cap, 5 * channels)),
            pl.BlockSpec((many, 3 * channels), lambda i: (i, 0)),
            pl.BlockSpec((many, latent_width), lambda i: (i, 0)),
            whole(scalar_proj.shape),
            whole(path_gain.shape),
            whole((1, latent_width)),
        ],
        out_specs=(
            pl.BlockSpec((many, latent_width), lambda i: (i, 0)),
            pl.BlockSpec((3, many, channels), lambda i: (0, i, 0)),
            whole((owners, atoms // LANES, LANES)),
        ),
        scratch_shapes=[
            pltpu.VMEM((owners * window, 5 * channels), bf16),
            pltpu.VMEM((many, 5 * channels), f32),
            pltpu.VMEM((atoms, LANES), f32),
        ],
        compiler_params=pltpu.CompilerParams(dimension_semantics=("arbitrary",)),
        name="final",
    )(
        starts,
        rows,
        received,
        mixed,
        latent,
        scalar_proj,
        path_gain,
        energy_proj.reshape(1, latent_width),
    )
    sums = lax.all_to_all(sums, ("gy", "gz"), split_axis=0, concat_axis=0, tiled=True)
    return (latent_out, vector_out, jnp.sum(sums, axis=0).reshape(atoms))


def solution(mesh):
    placed = (
        P(("gx", "gy", "gz"), None),
        P(("gx", "gy", "gz"), None, None),
        P(("gx", "gy", "gz")),
        P(None, ("gx", "gy", "gz")),
        P(("gx", "gy", "gz")),
        P(("gx", "gy", "gz"), None),
        P(("gx", "gy", "gz")),
        P(("gx", "gy", "gz")),
        P(),
        P(),
        P(),
        P(),
        P(),
        P(),
        P(),
        P(),
    )

    return jax.shard_map(
        local,
        mesh=mesh,
        in_specs=placed,
        out_specs=(
            P(("gx", "gy", "gz"), None),
            P(None, ("gx", "gy", "gz"), None),
            P(("gx", "gy", "gz")),
        ),
        check_vma=False,
    )
```
